32 devices in a mesh: member: 4 (over y, x), dom: 8 (over z, core).
Axes of the slice: x: 2, y: 2, z: 4, core: 2. Of those that a mesh axis runs over, the one named last changes fastest.
Arguments:
- acoustic_perturbation: float32 [4, 32, 8192], P('member', None, 'dom'), may hold values from -8 to 8
- prior_acoustic_state: float32 [4, 32, 8192], P('member', None, 'dom'), may hold values from -8 to 8
- thermal_anomaly: float32 [4, 32, 8192], P('member', None, 'dom'), may hold values from -8 to 8
- model_parameters: float32 [4, 4], P('member'), may hold values from 0.5 to 1.5
- crossing_velocity: float32 [32, 24576], P(None, 'dom'), may hold values from -3 to 3
- face_extent: float32 [24576], P('dom'), may hold values from 0.1 to 0.4
- face_metric_factor: float32 [24576], P('dom'), may hold values from 0.01 to 0.06
- reciprocal_polygon_surface: float32 [8192], P('dom'), may hold values from 0.5 to 2
- owned_totals: int32 [8], P('dom'), may hold values from 768 to 1024, as said below
- export_lists: int32 [8, 6, 128], P('dom'), may hold values from 0 to 1024, as said below
- face_neighbour_pair: int32 [2, 24576], P(None, 'dom'), may hold values from 0 to 1792, as said below
- polygon_side_lookup: int32 [6, 8192], P(None, 'dom'), may hold values from 0 to 3072, as said below
Outputs:
- pressure_out: float32 [4, 32, 8192], P('member', None, 'dom')
- temperature_out: float32 [4, 32, 8192], P('member', None, 'dom')
- ensemble_mean: float32 [32, 8192], P(None, 'dom')
The draws below stay inside these ranges and needn't reach their ends.
Inputs may be any that keep to these rules, and one draw needn't show every extreme that they name: The first owned_totals[p] cell slots of partition p are its cells, the rest unused; some partition has 1024. Row export_lists[p, b] lists owned cells of partition p sent to partition (p + offsets[b]) mod 8; filled entries first, then 1024 in the empty slots; at least 64 filled entries a row; in every draw some partition receives 128 filled entries in all 6 of its rows. `face_neighbour_pair`: edge 3 i + j of partition p starts at owned cell i and ends at another owned cell or at halo column 1024 + b * 128 + k whose slot k is filled in the sender's row b; edges of unused cells have both ends at 1792. `polygon_side_lookup`: the local edges with an end at each owned cell, 3072 in empty slots; unused cells have only empty slots.
All inputs are finite; a program needn't handle non-finite values.
Results may differ from the reference program's by a relative error of at most 0.0001.
Values sent between devices are 32-bit elements; how exact they have to be, the bound alone decides.
A program may use at most 64 MiB of HBM per device.

```python
import math
import jax
import jax.numpy as jnp

DOMAIN_CAPACITY = 1024
VERTICAL_LAYERS = 32
HB = 128
NB = 6
MAXE = 6
STEPS = 2
NS = 3
E_DEV = 3072
CELLS = 8192
EDGES = 24576
MEMBERS = 4
N_DOM = 8


def neighbour_offsets_drawn(count):
    return [(block_number // 2 + 1) * (1 - 2 * (block_number % 2)) for block_number in range(count)]


def mesh_tables(key):
    keys = jax.random.split(jax.random.fold_in(key, 7), 9)
    cell_counts = jax.random.randint(keys[0], (N_DOM,), 3 * DOMAIN_CAPACITY // 4, DOMAIN_CAPACITY + 1)
    full_part = jax.random.randint(keys[1], (), 0, N_DOM)
    cell_counts = cell_counts.at[full_part].set(DOMAIN_CAPACITY).astype(jnp.int32)
    offsets = jnp.array(neighbour_offsets_drawn(NB), jnp.int32)
    block_ids = jnp.arange(NB, dtype=jnp.int32)
    filled = jax.random.randint(keys[2], (N_DOM, NB), HB // 2, HB + 1)
    receiver = jax.random.randint(keys[3], (), 0, N_DOM)
    senders = (receiver - offsets) % N_DOM
    filled = filled.at[senders, block_ids].set(HB)
    slot_ids = jnp.arange(HB, dtype=jnp.int32)
    send_raw = jax.random.randint(keys[4], (N_DOM, NB, HB), 0, cell_counts[:, None, None])
    send_table = jnp.where(slot_ids[None, None, :] < filled[:, :, None], send_raw, DOMAIN_CAPACITY).astype(jnp.int32)
    part_ids = jnp.arange(N_DOM, dtype=jnp.int32)
    filled_in = filled[(part_ids[:, None] - offsets[None, :]) % N_DOM, block_ids[None, :]]
    cell_ids = jnp.arange(DOMAIN_CAPACITY, dtype=jnp.int32)
    halo_flag = jax.random.randint(keys[5], (N_DOM, DOMAIN_CAPACITY, 3), 0, 2)
    shifts = jax.random.randint(keys[6], (N_DOM, 3), 1, cell_counts[:, None])
    local_end = (cell_ids[None, :, None] + shifts[:, None, :]) % cell_counts[:, None, None]
    halo_block = jax.random.randint(keys[7], (N_DOM, DOMAIN_CAPACITY, 3), 0, NB)
    block_fill = filled_in[part_ids[:, None, None], halo_block]
    halo_slot = jax.random.randint(keys[8], (N_DOM, DOMAIN_CAPACITY, 3), 0, block_fill)
    halo_end = DOMAIN_CAPACITY + halo_block * HB + halo_slot
    valid = cell_ids[None, :, None] < cell_counts[:, None, None]
    zero_col = DOMAIN_CAPACITY + NB * HB
    start_cell = jnp.where(valid, cell_ids[None, :, None] + 0 * halo_flag, zero_col)
    end_cell = jnp.where(valid, jnp.where(halo_flag == 1, halo_end, local_end), zero_col)
    edge_table = jnp.stack([start_cell.reshape(N_DOM, E_DEV), end_cell.reshape(N_DOM, E_DEV)]).reshape(2, EDGES).astype(jnp.int32)
    side_ids = jnp.arange(3, dtype=jnp.int32)
    outgoing = jnp.where(valid, 3 * cell_ids[None, :, None] + side_ids[None, None, :], E_DEV)
    source = (cell_ids[None, :, None] - shifts[:, None, :]) % cell_counts[:, None, None]
    source_flag = jnp.take_along_axis(halo_flag, source, axis=1)
    incoming = jnp.where(valid & (source_flag == 0), 3 * source + side_ids[None, None, :], E_DEV)
    incidence = jnp.concatenate([outgoing, incoming], axis=2)
    incidence = jnp.transpose(incidence, (2, 0, 1)).reshape(MAXE, CELLS).astype(jnp.int32)
    return (cell_counts, send_table, edge_table, incidence)


def draw_owned_totals(key, part):
    return mesh_tables(key)[0]


def draw_export_lists(key, part):
    return mesh_tables(key)[1]


def draw_face_neighbour_pair(key, part):
    return mesh_tables(key)[2]


def draw_polygon_side_lookup(key, part):
    return mesh_tables(key)[3]


def regional_field(key):
    keys = jax.random.split(key, 2)
    region = 1.5 * jax.random.normal(keys[0], (MEMBERS, 1, N_DOM, 1), jnp.float32)
    noise = jax.random.normal(keys[1], (MEMBERS, VERTICAL_LAYERS, N_DOM, DOMAIN_CAPACITY), jnp.float32)
    return jnp.clip(region + noise, -8.0, 8.0).reshape(MEMBERS, VERTICAL_LAYERS, CELLS)


def draw_acoustic_perturbation(key, part):
    return regional_field(jax.random.fold_in(key, 11))


def draw_prior_acoustic_state(key, part):
    base = regional_field(jax.random.fold_in(key, 11))
    jitter = 0.3 * jax.random.normal(jax.random.fold_in(key, 12), (MEMBERS, VERTICAL_LAYERS, CELLS), jnp.float32)
    return jnp.clip(base + jitter, -8.0, 8.0)


def draw_thermal_anomaly(key, part):
    return regional_field(jax.random.fold_in(key, 13))


def levels(rng, dims, shards, smallest, top_value):
    level, own = 1.0, jax.random.fold_in(rng, 6)
    for dim, parts in shards:
        steps = jnp.exp(jax.random.uniform(jax.random.fold_in(own, dim), (parts,), jnp.float32, smallest / len(shards), top_value / len(shards)))
        level = level * jnp.repeat(steps, dims[dim] // parts).reshape([-1 if axis == dim else 1 for axis in range(len(dims))])
    return level


def centred(stream_key, extent, deviation, most, shards=(), held_as=jnp.bfloat16):
    factor_of = levels(stream_key, extent, shards, -0.22, 0.18) if shards else 1.0
    values = jax.random.normal(stream_key, extent, jnp.float32) * deviation * factor_of
    return jnp.minimum(jnp.maximum(values, -most), most).astype(held_as)


def setup_inputs(seed: int = 0) -> dict:
    key_list = jax.random.split(jax.random.key(seed), 13)
    acoustic_perturbation = draw_acoustic_perturbation(jax.random.fold_in(key_list[12], 71), 0)
    prior_acoustic_state = draw_prior_acoustic_state(jax.random.fold_in(key_list[12], 71), 0)
    thermal_anomaly = draw_thermal_anomaly(jax.random.fold_in(key_list[12], 71), 0)
    model_parameters = jnp.clip(0.5 + 1.0 * jax.random.uniform(key_list[3], (MEMBERS, 4), jnp.float32) ** levels(key_list[3], (MEMBERS, 4), ((0, 4),), -0.2, 0.2), 0.5, 1.5)
    crossing_velocity = centred(key_list[4], (VERTICAL_LAYERS, EDGES), 0.5, 3.0, ((1, 8),), jnp.float32)
    face_extent = jnp.clip(jnp.exp(math.log(0.4) - 1.3862944 * jax.random.uniform(key_list[5], (EDGES,), jnp.float32) ** levels(key_list[5], (EDGES,), ((0, 8),), -0.2, 0.2)), 0.1, 0.4)
    face_metric_factor = jnp.clip(jnp.exp(math.log(0.06) - 1.7917595 * jax.random.uniform(key_list[6], (EDGES,), jnp.float32) ** levels(key_list[6], (EDGES,), ((0, 8),), -0.2, 0.2)), 0.01, 0.06)
    reciprocal_polygon_surface = jnp.clip(jnp.exp(math.log(2.0) - 1.3862944 * jax.random.uniform(key_list[7], (CELLS,), jnp.float32) ** levels(key_list[7], (CELLS,), ((0, 8),), -0.2, 0.2)), 0.5, 2.0)
    owned_totals = draw_owned_totals(jax.random.fold_in(key_list[12], 71), 0)
    export_lists = draw_export_lists(jax.random.fold_in(key_list[12], 71), 0)
    face_neighbour_pair = draw_face_neighbour_pair(jax.random.fold_in(key_list[12], 71), 0)
    polygon_side_lookup = draw_polygon_side_lookup(jax.random.fold_in(key_list[12], 71), 0)
    return dict(acoustic_perturbation=acoustic_perturbation, prior_acoustic_state=prior_acoustic_state, thermal_anomaly=thermal_anomaly, model_parameters=model_parameters, crossing_velocity=crossing_velocity, face_extent=face_extent, face_metric_factor=face_metric_factor, reciprocal_polygon_surface=reciprocal_polygon_surface, owned_totals=owned_totals, export_lists=export_lists, face_neighbour_pair=face_neighbour_pair, polygon_side_lookup=polygon_side_lookup)


time_step = 0.25


def neighbour_offsets(count):
    return [(block_number // 2 + 1) * (1 - 2 * (block_number % 2)) for block_number in range(count)]


def extend_all(fields, export_lists):
    row_count = fields.shape[0]
    zero_column = jnp.zeros((row_count, N_DOM, 1), jnp.float32)
    padded_fields = jnp.concatenate([fields, zero_column], axis=2)
    pieces = [fields]
    for block_number, offset in enumerate(neighbour_offsets(NB)):
        sources = ((jnp.arange(N_DOM, dtype=jnp.int32) - offset) % N_DOM).astype(jnp.int32)
        chosen = export_lists[sources, block_number, :]
        pieces.append(jnp.take_along_axis(padded_fields[:, sources, :], chosen[None], axis=2))
    pieces.append(zero_column)
    return jnp.concatenate(pieces, axis=2)


def at_cells(extended, cell_list):
    return jnp.take_along_axis(extended, cell_list[None], axis=2)


def divergence_all(fluxes, polygon_side_lookup, edge_sign):
    padded_flux = jnp.concatenate([fluxes, jnp.zeros((fluxes.shape[0], N_DOM, 1), jnp.float32)], axis=2)
    summed = jnp.zeros((fluxes.shape[0], N_DOM, DOMAIN_CAPACITY), jnp.float32)
    for corner in range(MAXE):
        summed = summed + edge_sign[corner][None] * at_cells(padded_flux, polygon_side_lookup[corner])
    return summed


def reference(acoustic_perturbation, prior_acoustic_state, thermal_anomaly, model_parameters, crossing_velocity, face_extent, face_metric_factor, reciprocal_polygon_surface, owned_totals, export_lists, face_neighbour_pair, polygon_side_lookup):
    wind = crossing_velocity.reshape(VERTICAL_LAYERS, N_DOM, E_DEV)
    lengths = face_extent.reshape(N_DOM, E_DEV)[None]
    weights = face_metric_factor.reshape(N_DOM, E_DEV)[None]
    inverse = reciprocal_polygon_surface.reshape(N_DOM, DOMAIN_CAPACITY)[None]
    ends = face_neighbour_pair.reshape(2, N_DOM, E_DEV)
    incident = polygon_side_lookup.reshape(MAXE, N_DOM, DOMAIN_CAPACITY)
    cell_ids = jnp.arange(DOMAIN_CAPACITY, dtype=jnp.int32)
    owned = (cell_ids[None, :] < owned_totals[:, None])[None]
    cell_area = jnp.where(owned, 1.0 / inverse, jnp.float32(0.0))
    starts_padded = jnp.concatenate([ends[0], jnp.full((N_DOM, 1), -1, jnp.int32)], axis=1)
    edge_sign = jnp.stack([
        jnp.where(jnp.take_along_axis(starts_padded, incident[corner], axis=1) == cell_ids[None, :], jnp.float32(1.0), jnp.float32(-1.0))
        for corner in range(MAXE)])
    press_list, temp_list = [], []
    for perturbed_run in range(MEMBERS):
        speed = model_parameters[perturbed_run, 0]
        kappa = 0.5 * model_parameters[perturbed_run, 1]
        mixing = 0.6 * model_parameters[perturbed_run, 2]
        couple = model_parameters[perturbed_run, 3]
        current = acoustic_perturbation[perturbed_run].reshape(VERTICAL_LAYERS, N_DOM, DOMAIN_CAPACITY)
        previous = prior_acoustic_state[perturbed_run].reshape(VERTICAL_LAYERS, N_DOM, DOMAIN_CAPACITY)
        scalar_quantity = thermal_anomaly[perturbed_run].reshape(VERTICAL_LAYERS, N_DOM, DOMAIN_CAPACITY)
        for outer_step in range(STEPS):
            theta_ext = extend_all(scalar_quantity, export_lists)
            left = at_cells(theta_ext, ends[0])
            right = at_cells(theta_ext, ends[1])
            fluxes = lengths * (0.5 * wind * (left + right) - (0.5 * jnp.abs(wind) + kappa) * (right - left))
            differences = scalar_quantity[1:] - scalar_quantity[:-1]
            zero_row = jnp.zeros((1, N_DOM, DOMAIN_CAPACITY), jnp.float32)
            vertical = mixing * (jnp.concatenate([differences, zero_row], 0) - jnp.concatenate([zero_row, differences], 0))
            advanced = jnp.where(owned, scalar_quantity + time_step * (-inverse * divergence_all(fluxes, incident, edge_sign) + vertical), scalar_quantity)
            forcing = couple * (advanced - scalar_quantity) / NS
            for substep in range(NS):
                press_ext = extend_all(current, export_lists)
                gradient = weights * (at_cells(press_ext, ends[1]) - at_cells(press_ext, ends[0]))
                stepped = jnp.where(owned, 2.0 * current - previous + speed * inverse * divergence_all(gradient, incident, edge_sign) + forcing, current)
                previous, current = current, stepped
            level_mean = (jnp.sum(current * cell_area, axis=(1, 2)) / jnp.sum(cell_area))[:, None, None]
            current = jnp.where(owned, current - level_mean, current)
            previous = jnp.where(owned, previous - level_mean, previous)
            scalar_quantity = advanced
        press_list.append(current.reshape(VERTICAL_LAYERS, CELLS))
        temp_list.append(scalar_quantity.reshape(VERTICAL_LAYERS, CELLS))
    press_all = jnp.stack(press_list)
    temp_all = jnp.stack(temp_list)
    return press_all, temp_all, jnp.sum(press_all, axis=0) / MEMBERS
```

```python
import functools

import jax
import jax.numpy as jnp
from jax import lax
from jax.experimental import pallas as pl
from jax.experimental.pallas import tpu as pltpu
from jax.sharding import PartitionSpec as P

STEPS = 2
NS = 3
TIME_STEP = 0.25
LANES = 128
CHUNKS = 2
MESH = pl.DeviceIdType.MESH
F32 = jnp.float32
BF16 = jnp.bfloat16
F8 = jnp.float8_e4m3fn
I8 = jnp.int8
scope = jax.named_scope


def neighbour_offsets(count):
    return [(b // 2 + 1) * (1 - 2 * (b % 2)) for b in range(count)]


def mm(a, b):
    return jnp.dot(a, b, preferred_element_type=F32)


def mm_nt(a, b):
    return lax.dot_general(a, b, (((1,), (1,)), ((), ())), preferred_element_type=F32)


def halves(x):
    high = x.astype(BF16)
    low = (x - high.astype(F32)).astype(BF16)
    return jnp.concatenate([high, low], axis=0)


def fold(x):
    rows = x.shape[0] // 2
    return x[:rows] + x[rows:]


def one_hot(dst, row_blocks, columns, row_of):
    width = 512 if columns % 512 == 0 else 256 if columns % 256 == 0 else LANES

    def body(b, carry):
        for at in range(0, columns, width):
            cut = slice(at, at + width)
            row = row_of(cut)
            near = jnp.where((row >> 7) == b, row & (LANES - 1), -1)
            near = jnp.broadcast_to(near, (32, width)).astype(I8)
            for s in range(0, LANES, 32):
                rows = (lax.broadcasted_iota(jnp.int32, (32, width), 0) + s).astype(I8)
                dst[pl.ds(pl.multiple_of(b * LANES + s, 32), 32), cut] = jnp.where(
                    rows == near, F8(1), F8(0)
                )
        return carry

    lax.fori_loop(0, row_blocks, body, 0)


def kernel(
    n,
    members,
    par_hbm,
    p_hbm,
    q_hbm,
    t_hbm,
    v_hbm,
    ext_hbm,
    met_hbm,
    inv_hbm,
    exp_hbm,
    fin_hbm,
    p_hold,
    t_hold,
    e_hold,
    par_ref,
    p_out,
    t_out,
    e_out,
    p_ref,
    q_ref,
    t_ref,
    v_ref,
    ext_ref,
    met_ref,
    inv_ref,
    exp_ref,
    fin_ref,
    in_sem,
    out_sem,
    pick,
    g,
    m3,
    tab,
    itab,
    ej,
    endj,
    ends_s,
    cf,
    ct,
    send,
    recv,
    mean_send,
    mean_recv,
    mem_send,
    mem_recv,
    mm_send,
    mm_recv,
    w_send,
    w_recv,
    send_sem,
    recv_sem,
    mean_ssem,
    mean_rsem,
    mem_ssem,
    mem_rsem,
    mm_sem,
    w_sem,
):
    levels, cells = p_ref.shape[1], p_ref.shape[2]
    slabs = v_ref.shape[1] // cells
    blocks = cells // LANES
    nb, hb = send.shape[1], send.shape[3]
    halo = nb * hb
    me = lax.axis_index("dom")
    mine = lax.axis_index("member")
    offsets = neighbour_offsets(nb)
    stages = members.bit_length() - 1

    def dom_peer(k):
        return {"dom": lax.rem(me + (k % n), n)}

    def member_peer(k):
        return {"member": lax.rem(mine + (k % members), members)}

    def partner(stage):
        bit = 1 << stage
        return {"member": mine + bit - 2 * bit * lax.rem(mine // bit, 2)}

    with scope("start"):
        barrier = pltpu.get_barrier_semaphore()
        for k in range(1, n):
            pl.semaphore_signal(barrier, inc=1, device_id=dom_peer(k), device_id_type=MESH)
        for k in range(1, members):
            pl.semaphore_signal(barrier, inc=1, device_id=member_peer(k), device_id_type=MESH)
        loads = {}
        for at, (name, src, dst) in enumerate(
            [
                ("exp", exp_hbm, exp_ref),
                ("t", t_hbm, t_ref),
                ("p", p_hbm, p_ref),
                ("fin", fin_hbm, fin_ref),
                ("par", par_hbm, par_ref),
                ("met", met_hbm, met_ref),
                ("inv", inv_hbm, inv_ref),
                ("ext", ext_hbm, ext_ref),
                ("v", v_hbm, v_ref),
                ("q", q_hbm, q_ref),
            ]
        ):
            loads[name] = pltpu.make_async_copy(src, dst, in_sem.at[at])
            loads[name].start()


    def to_peer(src, dst, send_sem, recv_sem, peer):
        return pltpu.make_async_remote_copy(
            src_ref=src,
            dst_ref=dst,
            send_sem=send_sem,
            recv_sem=recv_sem,
            device_id=peer,
            device_id_type=MESH,
        )

    def exchange(slot, chosen):
        for b, offset in enumerate(offsets):
            send[slot, b] = chosen[:, b * hb : (b + 1) * hb]
            to_peer(
                send.at[slot, b],
                recv.at[slot, b],
                send_sem.at[0],
                recv_sem.at[slot],
                dom_peer(offset),
            ).start()

    def arrived(slot):
        to_peer(
            send.at[slot], recv.at[slot], send_sem.at[0], recv_sem.at[slot], dom_peer(1)
        ).wait_recv()
        return halves(jnp.concatenate([recv[slot, b] for b in range(nb)], axis=1))

    def chosen_of(*fields):
        y = mm(jnp.concatenate([halves(x) for x in fields], axis=0), pick[...])
        return [fold(y[2 * levels * i : 2 * levels * (i + 1)]) for i in range(len(fields))]

    with scope("pick_build"):
        loads["exp"].wait()
        one_hot(pick, blocks, halo, lambda cut: exp_ref[0:1, cut])
    with scope("pick0"):
        loads["t"].wait()
        loads["p"].wait()
        current = p_ref[0]
        theta = t_ref[0]
        theta_s, current_s = chosen_of(theta, current)

    with scope("tables"):
        loads["fin"].wait()
        loads["met"].wait()
        loads["inv"].wait()
        loads["ext"].wait()
        loads["par"].wait()
        speed = par_ref[0, 0]
        kappa = 0.5 * par_ref[0, 1]
        mixing = 0.6 * par_ref[0, 2]
        couple = par_ref[0, 3]
        tab[0:8, :] = jnp.broadcast_to(met_ref[...], (8, slabs * cells))
        tab[8:16, :] = jnp.broadcast_to(ext_ref[...], (8, slabs * cells))
        itab[...] = jnp.broadcast_to(fin_ref[1:2, :], (8, slabs * cells))

        def slab(ref, rows, b, j):
            at = slabs * lax.broadcasted_iota(jnp.int32, (rows, LANES), 1) + j
            block, lane = at >> 7, at & (LANES - 1)
            out = None
            for s in range(slabs):
                lo = (slabs * b + s) * LANES
                y = jnp.take_along_axis(
                    ref[0:rows, lo : lo + LANES], lane, axis=1, mode="promise_in_bounds"
                )
                out = y if out is None else jnp.where(block == s, y, out)
            return out

        for b in range(blocks):
            for j in range(slabs):
                lo = j * cells + b * LANES
                ej[:, lo : lo + LANES] = slab(tab, 16, b, j)
                endj[:, lo : lo + LANES] = slab(itab, 8, b, j)
        inverse = inv_ref[...]
        owned = endj[0:1, :cells] < cells + halo
        area = jnp.where(owned, 1.0 / inverse, 0.0)
        scale = jnp.where(owned, speed * inverse, 0.0)
        rate = jnp.where(owned, TIME_STEP * inverse, 0.0)
    cuts = [slice(j * cells, (j + 1) * cells) for j in range(slabs)]
    metric = [ej[0:1, cut] for cut in cuts]
    extent = [ej[8:9, cut] for cut in cuts]

    with scope("bar_wait"):
        pl.semaphore_wait(barrier, n - 1 + members - 1)
    with scope("send0"):
        exchange(0, theta_s)
        exchange(1, current_s)

    with scope("g_build"):
        one_hot(g, (cells + halo) // LANES, slabs * cells, lambda cut: endj[0:1, cut])
    with scope("coef"):
        loads["v"].wait()
        for j in range(slabs):
            for b in range(blocks):
                lanes = slice(b * LANES, (b + 1) * LANES)
                wind = slab(v_ref, levels, b, j)
                down = extent[j][:, lanes] * (0.5 * wind - (0.5 * jnp.abs(wind) + kappa))
                cf[j, :, lanes] = down
                ct[j, :, lanes] = extent[j][:, lanes] * wind - down
    with scope("m3_build"):
        rows = [endj[0:1, cut].astype(F32) for cut in cuts] + [scale * m for m in metric]
        rows = jnp.concatenate(rows + [jnp.zeros((16 - 2 * slabs, cells), F32)], axis=0)
        y = fold(mm(halves(rows), pick[...]))
        for j in range(slabs):
            ends_s[0:1, j * halo : (j + 1) * halo] = y[j : j + 1].astype(jnp.int32) - cells
        weight_s = [y[slabs + j : slabs + j + 1] for j in range(slabs)]
        one_hot(m3, nb, slabs * halo, lambda cut: ends_s[0:1, cut])

    def local(pressure, heat=None):
        lhs = [halves(pressure)] + ([] if heat is None else [halves(heat)])
        lhs = jnp.concatenate(lhs, axis=0)
        p_flux, t_flux = [], []
        for j in range(slabs):
            y = mm(lhs, g[:cells, cuts[j]])
            p_flux.append(metric[j] * (fold(y[: 2 * levels]) - pressure))
            if heat is not None:
                t_flux.append(cf[j] * fold(y[2 * levels :]) + ct[j] * heat)
        lhs = [halves(jnp.concatenate(p_flux, axis=1))]
        if heat is not None:
            lhs.append(halves(jnp.concatenate(t_flux, axis=1)))
        y = mm_nt(jnp.concatenate(lhs, axis=0), g[:cells, :])
        p_sum = sum(p_flux[1:], p_flux[0]) - fold(y[: 2 * levels])
        if heat is None:
            return p_sum
        return p_sum, sum(t_flux[1:], t_flux[0]) - fold(y[2 * levels :])

    def far(x, j):
        return mm(x, g[cells:, cuts[j]])

    def far_s(x, j):
        return mm(x, m3[:, j * halo : (j + 1) * halo])

    def heat_base(heat, div):
        step = heat[1:] - heat[:-1]
        zero = jnp.zeros((1, cells), F32)
        vertical = mixing * (
            jnp.concatenate([step, zero], 0) - jnp.concatenate([zero, step], 0)
        )
        return heat + jnp.where(owned, TIME_STEP * vertical, 0.0) - rate * div

    def lane_blocks(x):
        parts = [x[:, b * LANES : (b + 1) * LANES] for b in range(x.shape[1] // LANES)]
        return sum(parts[1:], parts[0])

    def partial_mean(slot, weighted):
        weighted = jnp.sum(weighted, axis=1, keepdims=True)
        whole = jnp.sum(area, axis=1, keepdims=True)
        row_at = lax.broadcasted_iota(jnp.int32, (levels, LANES), 0)
        lane_at = lax.broadcasted_iota(jnp.int32, (levels, LANES), 1)
        row = jnp.sum(jnp.where(row_at == lane_at, weighted, 0.0), axis=0, keepdims=True)
        lane = lax.broadcasted_iota(jnp.int32, (1, LANES), 1)
        row = jnp.where(lane < levels, row, whole)
        mean_send[slot] = jnp.broadcast_to(row, (8, LANES))
        for k in range(1, n):
            to_peer(
                mean_send.at[slot],
                mean_recv.at[slot, k - 1],
                mean_ssem.at[0],
                mean_rsem.at[slot],
                dom_peer(k),
            ).start()

    def mean_row(slot):
        to_peer(
            mean_recv.at[slot],
            mean_recv.at[slot],
            mean_ssem.at[0],
            mean_rsem.at[slot],
            dom_peer(1),
        ).wait_recv()
        total = mean_send[slot]
        for k in range(n - 1):
            total = total + mean_recv[slot, k]
        return total / total[:, levels : levels + 1]

    def as_column(row):
        row_at = lax.broadcasted_iota(jnp.int32, (levels, LANES), 0)
        lane_at = lax.broadcasted_iota(jnp.int32, (levels, LANES), 1)
        return jnp.sum(jnp.where(row_at == lane_at, row[0:1], 0.0), axis=1, keepdims=True)

    with scope("local_0"):
        p_sum, t_sum = local(current, theta)
        loads["q"].wait()
        base = jnp.where(owned, 2.0 * current - q_ref[0], current) + scale * p_sum
        t_base = heat_base(theta, t_sum)
    with scope("base_0"):
        base_s, t_base_s, *turn_s = chosen_of(
            base, t_base, *[rate * cf[j] for j in range(slabs)]
        )
    with scope("wait_0"):
        ht = arrived(0)
        hp = arrived(1)
    share = couple / NS
    with scope("crit_0"):
        both = jnp.concatenate([ht, hp], axis=0)
        out, t_out_s = base_s, t_base_s
        for j in range(slabs):
            y = far_s(both, j)
            t_out_s = t_out_s - turn_s[j] * fold(y[: 2 * levels])
            out = out + weight_s[j] * fold(y[2 * levels :])
        out = out + share * (t_out_s - theta_s)
        exchange(2, out)
        exchange(STEPS * NS + 1, t_out_s)
    with scope("full_0"):
        theta1 = t_base
        previous, stepped = current, base
        for j in range(slabs):
            y = far(both, j)
            theta1 = theta1 - rate * (cf[j] * fold(y[: 2 * levels]))
            stepped = stepped + (scale * metric[j]) * fold(y[2 * levels :])
        forcing = share * (theta1 - theta)
        current = stepped + forcing

    def w_copy(b, offset):
        whole = offset == 0
        return to_peer(
            w_send if whole else w_send.at[b],
            w_recv if whole else w_recv.at[b],
            w_sem.at[0],
            w_sem.at[1],
            dom_peer(1 if whole else offset),
        )

    total = STEPS * NS
    for k in range(1, total):
        with scope(f"local_{k}"):
            if k == 1:
                p_sum, t_sum = local(current, theta1)
                t_base = heat_base(theta1, t_sum)
            else:
                p_sum = local(current)
            if k == NS - 1:
                ht = arrived(STEPS * NS + 1)
                theta2 = t_base
                for j in range(slabs):
                    theta2 = theta2 - rate * (cf[j] * fold(far(ht, j)))
                t_out[0] = theta2
                t_copy = pltpu.make_async_copy(t_out, t_hold, out_sem.at[0])
                t_copy.start()
            if k == NS:
                forcing = share * (theta2 - theta1)
                partial_mean(0, lane_blocks(current * area))
            base = (
                jnp.where(owned, 2.0 * current - previous, current) + scale * p_sum + forcing
            )
        if k < total - 1:
            with scope(f"base_{k}"):
                (base_s,) = chosen_of(base)
        else:
            with scope("mean_1"):
                w_copy(0, 0).wait_recv()
                weighted = lane_blocks(base * area)
                for b in range(nb):
                    weighted = weighted + w_recv[b, 0:1] * send[k + 1, b]
                partial_mean(1, weighted)
                first_row = mean_row(0)
                first = as_column(first_row)
        if k == NS:
            with scope("pull"):
                rows = jnp.concatenate(
                    [speed * m for m in metric], axis=1
                )
                rows = halves(jnp.broadcast_to(rows, (16, slabs * cells)))
                w = fold(mm_nt(rows, g[cells:, :]))
                for b, offset in enumerate(offsets):
                    w_send[b] = w[0:8, b * hb : (b + 1) * hb]
                    w_copy(b, -offset).start()
        with scope(f"wait_{k}"):
            hp = arrived(k + 1)
        if k < total - 1:
            with scope(f"crit_{k}"):
                out = base_s
                for j in range(slabs):
                    out = out + weight_s[j] * fold(far_s(hp, j))
                exchange(k + 2, out)
        with scope(f"full_{k}"):
            previous, stepped = current, base
            for j in range(slabs):
                stepped = stepped + (scale * metric[j]) * fold(far(hp, j))
            current = stepped

    with scope("tail_send"):
        current = jnp.where(owned, current - first, current)
        pieces = max(stages, 1) * CHUNKS
        width = cells // pieces

        def member_copy(stage, c):
            return to_peer(
                mem_send.at[stage, c],
                mem_recv.at[stage, c],
                mem_ssem.at[0],
                mem_rsem.at[stage, c],
                partner((stage + c) % max(stages, 1)),
            )

        def row_copy(k):
            return to_peer(
                mm_send, mm_recv.at[k - 1], mm_sem.at[0], mm_sem.at[1], member_peer(k)
            )

        for c in range(pieces):
            mem_send[0, c] = current[:, c * width : (c + 1) * width]
            if stages:
                member_copy(0, c).start()
    with scope("tail_mean"):
        last = mean_row(1) - first_row
        mm_send[...] = last
        for k in range(1, members):
            row_copy(k).start()
        column = as_column(last)
        p_out[0] = jnp.where(owned, current - column, current)
        p_copy = pltpu.make_async_copy(p_out, p_hold, out_sem.at[1])
        p_copy.start()
    for s in range(stages - 1):
        with scope(f"tail_stage_{s}"):
            for c in range(pieces):
                member_copy(s, c).wait_recv()
                mem_send[s + 1, c] = mem_send[s, c] + mem_recv[s, c]
                member_copy(s + 1, c).start()
    with scope("tail_rows"):
        summed = last
        if members > 1:
            to_peer(mm_recv, mm_recv, mm_sem.at[0], mm_sem.at[1], member_peer(1)).wait_recv()
            for k in range(members - 1):
                summed = summed + mm_recv[k]
        column = as_column(summed)
    with scope("tail_end"):
        for c in range(pieces):
            cut = slice(c * width, (c + 1) * width)
            field = mem_send[max(stages - 1, 0), c]
            if stages:
                member_copy(stages - 1, c).wait_recv()
                field = field + mem_recv[stages - 1, c]
            e_out[:, cut] = (field - jnp.where(owned[:, cut], column, 0.0)) / members
        e_copy = pltpu.make_async_copy(e_out, e_hold, out_sem.at[2])
        e_copy.start()
    with scope("drain"):
        to_peer(send, recv, send_sem.at[0], recv_sem.at[0], dom_peer(1)).wait_send()
        to_peer(mean_recv, mean_recv, mean_ssem.at[0], mean_rsem.at[0], dom_peer(1)).wait_send()
        w_copy(0, 0).wait_send()
        if stages:
            to_peer(
                mem_send, mem_recv, mem_ssem.at[0], mem_rsem.at[0, 0], partner(0)
            ).wait_send()
        if members > 1:
            to_peer(mm_recv, mm_recv, mm_sem.at[0], mm_sem.at[1], member_peer(1)).wait_send()
        t_copy.wait()
        p_copy.wait()
        e_copy.wait()


def finish(p_hold, t_hold, e_hold, p_out, t_out, e_out, sem):
    copies = [
        pltpu.make_async_copy(src, dst, sem.at[at])
        for at, (src, dst) in enumerate(
            [(p_hold, p_out), (t_hold, t_out), (e_hold, e_out)]
        )
    ]
    for copy in copies:
        copy.start()
    for copy in copies:
        copy.wait()


def solution(mesh):
    n = mesh.shape["dom"]
    members = mesh.shape["member"]

    def per_device(
        acoustic_perturbation,
        prior_acoustic_state,
        thermal_anomaly,
        model_parameters,
        crossing_velocity,
        face_extent,
        face_metric_factor,
        reciprocal_polygon_surface,
        owned_totals,
        export_lists,
        face_neighbour_pair,
        polygon_side_lookup,
    ):
        _, levels, cells = acoustic_perturbation.shape
        edges = face_extent.shape[0]
        slabs = edges // cells
        nb, hb = export_lists.shape[1:]
        halo = nb * hb
        stages = members.bit_length() - 1
        some = max(stages, 1)
        pieces = some * CHUNKS
        slots = STEPS * NS + 2
        hbm = pl.BlockSpec(memory_space=pl.ANY)
        dma = pltpu.SemaphoreType.DMA
        field = pltpu.VMEM((1, levels, cells), F32)
        shapes = (
            jax.ShapeDtypeStruct((1, levels, cells), F32),
            jax.ShapeDtypeStruct((1, levels, cells), F32),
            jax.ShapeDtypeStruct((levels, cells), F32),
        )
        held = pl.pallas_call(
            functools.partial(kernel, n, members),
            out_shape=shapes,
            in_specs=[hbm] * 10,
            out_specs=(hbm, hbm, hbm),
            scratch_shapes=[
                pltpu.SMEM((1, 4), F32),
                field,
                field,
                pltpu.VMEM((levels, cells), F32),
                field,
                field,
                field,
                pltpu.VMEM((levels, edges), F32),
                pltpu.VMEM((1, edges), F32),
                pltpu.VMEM((1, edges), F32),
                pltpu.VMEM((1, cells), F32),
                pltpu.VMEM((1, halo), jnp.int32),
                pltpu.VMEM((2, edges), jnp.int32),
                dma((10,)),
                dma((3,)),
                pltpu.VMEM((cells, halo), F8),
                pltpu.VMEM((cells + halo, edges), F8),
                pltpu.VMEM((halo, slabs * halo), F8),
                pltpu.VMEM((16, edges), F32),
                pltpu.VMEM((8, edges), jnp.int32),
                pltpu.VMEM((16, edges), F32),
                pltpu.VMEM((8, edges), jnp.int32),
                pltpu.VMEM((8, slabs * halo), jnp.int32),
                pltpu.VMEM((slabs, levels, cells), F32),
                pltpu.VMEM((slabs, levels, cells), F32),
                pltpu.VMEM((slots, nb, levels, hb), F32),
                pltpu.VMEM((slots, nb, levels, hb), F32),
                pltpu.VMEM((STEPS, 8, LANES), F32),
                pltpu.VMEM((STEPS, n - 1, 8, LANES), F32),
                pltpu.VMEM((some, pieces, levels, cells // pieces), F32),
                pltpu.VMEM((some, pieces, levels, cells // pieces), F32),
                pltpu.VMEM((8, LANES), F32),
                pltpu.VMEM((max(members - 1, 1), 8, LANES), F32),
                pltpu.VMEM((nb, 8, hb), F32),
                pltpu.VMEM((nb, 8, hb), F32),
                dma((1,)),
                dma((slots,)),
                dma((1,)),
                dma((STEPS,)),
                dma((1,)),
                dma((some, pieces)),
                dma((2,)),
                dma((2,)),
            ],
            compiler_params=pltpu.CompilerParams(
                collective_id=0, has_side_effects=True, vmem_limit_bytes=32 * 1024 * 1024
            ),
        )(
            *[
                pltpu.with_memory_space_constraint(x, pltpu.HBM)
                for x in (
                    model_parameters,
                    acoustic_perturbation,
                    prior_acoustic_state,
                    thermal_anomaly,
                    crossing_velocity,
                    face_extent[None],
                    face_metric_factor[None],
                    reciprocal_polygon_surface[None],
                    export_lists.reshape(1, halo),
                    face_neighbour_pair,
                )
            ],
        )
        return pl.pallas_call(
            finish,
            out_shape=shapes,
            in_specs=[hbm] * 3,
            out_specs=(hbm, hbm, hbm),
            scratch_shapes=[dma((3,))],
            compiler_params=pltpu.CompilerParams(vmem_limit_bytes=1024 * 1024),
        )(*held)

    in_specs = (
        P("member", None, "dom"),
        P("member", None, "dom"),
        P("member", None, "dom"),
        P("member", None),
        P(None, "dom"),
        P("dom"),
        P("dom"),
        P("dom"),
        P("dom"),
        P("dom", None, None),
        P(None, "dom"),
        P(None, "dom"),
    )
    out_specs = (P("member", None, "dom"), P("member", None, "dom"), P(None, "dom"))
    return jax.shard_map(
        per_device, mesh=mesh, in_specs=in_specs, out_specs=out_specs, check_vma=False
    )
```

```python
import functools

import jax
import jax.numpy as jnp
from jax import lax
from jax.experimental import pallas as pl
from jax.experimental.pallas import tpu as pltpu
from jax.sharding import PartitionSpec as P

STEPS = 2
NS = 3
TIME_STEP = 0.25
LANES = 128
CHUNKS = 4
GROUP = 2
MESH = pl.DeviceIdType.MESH
F32 = jnp.float32
BF16 = jnp.bfloat16
F8 = jnp.float8_e4m3fn
I8 = jnp.int8
scope = jax.named_scope


def neighbour_offsets(count):
    return [(b // 2 + 1) * (1 - 2 * (b % 2)) for b in range(count)]


def mm(a, b):
    return jnp.dot(a, b, preferred_element_type=F32)


def mm_nt(a, b):
    return lax.dot_general(a, b, (((1,), (1,)), ((), ())), preferred_element_type=F32)


def halves(x):
    high = x.astype(BF16)
    low = (x - high.astype(F32)).astype(BF16)
    return jnp.concatenate([high, low], axis=0)


def fold(x):
    rows = x.shape[0] // 2
    return x[:rows] + x[rows:]


def one_hot(dst, row_blocks, columns, row_of):
    width = 512 if columns % 512 == 0 else 256 if columns % 256 == 0 else LANES

    def body(b, carry):
        for at in range(0, columns, width):
            cut = slice(at, at + width)
            row = row_of(cut)
            near = jnp.where((row >> 7) == b, row & (LANES - 1), -1)
            near = jnp.broadcast_to(near, (32, width)).astype(I8)
            for s in range(0, LANES, 32):
                rows = (lax.broadcasted_iota(jnp.int32, (32, width), 0) + s).astype(I8)
                dst[pl.ds(pl.multiple_of(b * LANES + s, 32), 32), cut] = jnp.where(
                    rows == near, F8(1), F8(0)
                )
        return carry

    lax.fori_loop(0, row_blocks, body, 0)


def kernel(
    n,
    members,
    par_hbm,
    p_hbm,
    q_hbm,
    t_hbm,
    v_hbm,
    ext_hbm,
    met_hbm,
    inv_hbm,
    exp_hbm,
    fin_hbm,
    p_hold,
    t_hold,
    e_hold,
    par_ref,
    p_out,
    t_out,
    e_out,
    p_ref,
    q_ref,
    t_ref,
    v_ref,
    ext_ref,
    met_ref,
    inv_ref,
    exp_ref,
    fin_ref,
    in_sem,
    out_sem,
    exp_s,
    pick,
    g,
    m3,
    tab,
    itab,
    ej,
    endj,
    ends_s,
    cf,
    ct,
    send,
    recv,
    mean_send,
    mean_recv,
    mem_send,
    mem_recv,
    mm_send,
    mm_recv,
    w_send,
    w_recv,
    send_sem,
    recv_sem,
    mean_ssem,
    mean_rsem,
    mem_ssem,
    mem_rsem,
    mm_sem,
    w_sem,
):
    levels, cells = p_ref.shape[1], p_ref.shape[2]
    slabs = v_ref.shape[1] // cells
    blocks = cells // LANES
    nb, hb = send.shape[1], send.shape[3]
    halo = nb * hb
    me = lax.axis_index("dom")
    mine = lax.axis_index("member")
    stages = members.bit_length() - 1
    groups = nb // GROUP
    wide = GROUP * hb

    offsets = neighbour_offsets(nb)
    ahead = [o for o in sorted(offsets, reverse=True) if o > 0]
    behind = [o for o in sorted(offsets, reverse=True) if o < 0]
    out_offsets = behind[1:] + behind[:1] + ahead
    in_offsets = behind + ahead[-1:] + ahead[:-1]
    out_blocks = [offsets.index(o) for o in out_offsets]
    in_blocks = [offsets.index(o) for o in in_offsets]
    half = (n + 1) // 2
    upper = me // half

    def turned(block):
        return block + upper * (1 - 2 * (block % 2))

    def meet(offset, block, order):
        peer = lax.rem(me + offset * (1 - 2 * upper) + n * nb, n)
        other = peer // half
        differ = upper + other - 2 * upper * other
        here, there = order.index(block), order.index(block + 1 - 2 * (block % 2))
        return {"dom": peer}, here + differ * (there - here)

    out_to = [meet(o, b, in_blocks) for o, b in zip(out_offsets, out_blocks)]
    in_from = [meet(-o, b, out_blocks) for o, b in zip(in_offsets, in_blocks)]

    def dom_peer(k):
        return {"dom": lax.rem(me + (k % n), n)}

    def member_peer(k):
        return {"member": lax.rem(mine + (k % members), members)}

    def partner(stage):
        bit = 1 << stage
        return {"member": mine + bit - 2 * bit * lax.rem(mine // bit, 2)}

    with scope("start"):
        barrier = pltpu.get_barrier_semaphore()
        for k in range(1, n):
            pl.semaphore_signal(barrier, inc=1, device_id=dom_peer(k), device_id_type=MESH)
        for k in range(1, members):
            pl.semaphore_signal(barrier, inc=1, device_id=member_peer(k), device_id_type=MESH)
        loads = {}
        for at, (name, src, dst) in enumerate(
            [
                ("exp", exp_hbm, exp_ref),
                ("t", t_hbm, t_ref),
                ("p", p_hbm, p_ref),
                ("fin", fin_hbm, fin_ref),
                ("par", par_hbm, par_ref),
                ("met", met_hbm, met_ref),
                ("inv", inv_hbm, inv_ref),
                ("ext", ext_hbm, ext_ref),
                ("v", v_hbm, v_ref),
                ("q", q_hbm, q_ref),
            ]
        ):
            loads[name] = pltpu.make_async_copy(src, dst, in_sem.at[at])
            loads[name].start()


    def to_peer(src, dst, send_sem, recv_sem, peer):
        return pltpu.make_async_remote_copy(
            src_ref=src,
            dst_ref=dst,
            send_sem=send_sem,
            recv_sem=recv_sem,
            device_id=peer,
            device_id_type=MESH,
        )

    rows_of = [2] + [k % 2 for k in range(STEPS * NS)] + [3]

    def exchange(slot, parts):
        for t, (peer, place) in enumerate(out_to):
            at = t % GROUP * hb
            send[slot, t] = parts[t // GROUP][:, at : at + hb]
            to_peer(
                send.at[slot, t],
                recv.at[slot, place],
                send_sem.at[0],
                recv_sem.at[rows_of[slot], place // GROUP],
                peer,
            ).start()

    def arrived(slot, group):
        at = slice(group * GROUP, (group + 1) * GROUP)
        to_peer(
            send.at[slot, at],
            recv.at[slot, at],
            send_sem.at[0],
            recv_sem.at[rows_of[slot], group],
            dom_peer(1),
        ).wait_recv()
        return halves(
            jnp.concatenate([recv[slot, group * GROUP + i] for i in range(GROUP)], axis=1)
        )

    def parted(x):
        return [x[:, at : at + wide] for at in range(0, halo, wide)]

    def chosen_of(*fields):
        y = mm(jnp.concatenate([halves(x) for x in fields], axis=0), pick[...])
        return [fold(y[2 * levels * i : 2 * levels * (i + 1)]) for i in range(len(fields))]

    with scope("pick_build"):
        loads["exp"].wait()
        for t, block in enumerate(out_blocks):
            at = pl.multiple_of(turned(block) * hb, hb)
            exp_s[0:1, t * hb : (t + 1) * hb] = exp_ref[0:1, pl.ds(at, hb)]
        one_hot(pick, blocks, halo, lambda cut: exp_s[0:1, cut])
    with scope("pick0"):
        loads["t"].wait()
        loads["p"].wait()
        current = p_ref[0]
        theta = t_ref[0]
        theta_s, current_s = chosen_of(theta, current)

    with scope("tables"):
        loads["fin"].wait()
        loads["met"].wait()
        loads["inv"].wait()
        loads["ext"].wait()
        loads["par"].wait()
        speed = par_ref[0, 0]
        kappa = 0.5 * par_ref[0, 1]
        mixing = 0.6 * par_ref[0, 2]
        couple = par_ref[0, 3]
        tab[0:8, :] = jnp.broadcast_to(met_ref[...], (8, slabs * cells))
        tab[8:16, :] = jnp.broadcast_to(ext_ref[...], (8, slabs * cells))
        ends = fin_ref[1:2, :]
        block = (ends >> 7) - blocks
        block = block + upper * (1 - 2 * (block & 1))
        place = block
        for b in range(nb):
            place = jnp.where(block == b, in_blocks.index(b), place)
        inner = (ends >= cells) & (ends < cells + halo)
        ends = jnp.where(inner, cells + place * hb + (ends & (hb - 1)), ends)
        itab[...] = jnp.broadcast_to(ends, (8, slabs * cells))

        def slab(ref, rows, b, j):
            at = slabs * lax.broadcasted_iota(jnp.int32, (rows, LANES), 1) + j
            block, lane = at >> 7, at & (LANES - 1)
            out = None
            for s in range(slabs):
                lo = (slabs * b + s) * LANES
                y = jnp.take_along_axis(
                    ref[0:rows, lo : lo + LANES], lane, axis=1, mode="promise_in_bounds"
                )
                out = y if out is None else jnp.where(block == s, y, out)
            return out

        for b in range(blocks):
            for j in range(slabs):
                lo = j * cells + b * LANES
                ej[:, lo : lo + LANES] = slab(tab, 16, b, j)
                endj[:, lo : lo + LANES] = slab(itab, 8, b, j)
        inverse = inv_ref[...]
        owned = endj[0:1, :cells] < cells + halo
        area = jnp.where(owned, 1.0 / inverse, 0.0)
        scale = jnp.where(owned, speed * inverse, 0.0)
        rate = jnp.where(owned, TIME_STEP * inverse, 0.0)
    cuts = [slice(j * cells, (j + 1) * cells) for j in range(slabs)]
    metric = [ej[0:1, cut] for cut in cuts]
    extent = [ej[8:9, cut] for cut in cuts]

    with scope("bar_wait"):
        pl.semaphore_wait(barrier, n - 1 + members - 1)
    with scope("send0"):
        exchange(0, parted(theta_s))
        exchange(1, parted(current_s))

    with scope("g_build"):
        one_hot(g, (cells + halo) // LANES, slabs * cells, lambda cut: endj[0:1, cut])
    with scope("coef"):
        loads["v"].wait()
        for j in range(slabs):
            for b in range(blocks):
                lanes = slice(b * LANES, (b + 1) * LANES)
                wind = slab(v_ref, levels, b, j)
                down = extent[j][:, lanes] * (0.5 * wind - (0.5 * jnp.abs(wind) + kappa))
                cf[j, :, lanes] = down
                ct[j, :, lanes] = extent[j][:, lanes] * wind - down
    with scope("m3_build"):
        rows = [endj[0:1, cut].astype(F32) for cut in cuts] + [scale * m for m in metric]
        rows = jnp.concatenate(rows + [jnp.zeros((16 - 2 * slabs, cells), F32)], axis=0)
        y = fold(mm(halves(rows), pick[...]))
        for j in range(slabs):
            for at, part in enumerate(parted(y[j : j + 1])):
                lo = (at * slabs + j) * wide
                ends_s[0:1, lo : lo + wide] = part.astype(jnp.int32) - cells
        weight_s = [parted(y[slabs + j : slabs + j + 1]) for j in range(slabs)]
        one_hot(m3, nb, slabs * halo, lambda cut: ends_s[0:1, cut])

    def local(pressure, heat=None):
        lhs = [halves(pressure)] + ([] if heat is None else [halves(heat)])
        lhs = jnp.concatenate(lhs, axis=0)
        p_flux, t_flux = [], []
        for j in range(slabs):
            y = mm(lhs, g[:cells, cuts[j]])
            p_flux.append(metric[j] * (fold(y[: 2 * levels]) - pressure))
            if heat is not None:
                t_flux.append(cf[j] * fold(y[2 * levels :]) + ct[j] * heat)
        lhs = [halves(jnp.concatenate(p_flux, axis=1))]
        if heat is not None:
            lhs.append(halves(jnp.concatenate(t_flux, axis=1)))
        y = mm_nt(jnp.concatenate(lhs, axis=0), g[:cells, :])
        p_sum = sum(p_flux[1:], p_flux[0]) - fold(y[: 2 * levels])
        if heat is None:
            return p_sum
        return p_sum, sum(t_flux[1:], t_flux[0]) - fold(y[2 * levels :])

    def far(x, j):
        return mm(x, g[cells:, cuts[j]])

    def relay(slot, parts, weights):
        held = []
        for group in range(groups):
            x = arrived(slot, group)
            held.append(x)
            found = [
                mm(
                    x,
                    m3[
                        group * wide : (group + 1) * wide,
                        part * slabs * wide : (part + 1) * slabs * wide,
                    ],
                )
                for part in range(groups)
            ]
            for part, y in enumerate(found):
                y = fold(y)
                for j in range(slabs):
                    parts[part] = parts[part] + weights[j][part] * (
                        y[:, j * wide : (j + 1) * wide]
                    )
        return parts, jnp.concatenate(held, axis=1)

    def arrived_all(slot):
        return jnp.concatenate([arrived(slot, group) for group in range(groups)], axis=1)

    def heat_base(heat, div):
        step = heat[1:] - heat[:-1]
        zero = jnp.zeros((1, cells), F32)
        vertical = mixing * (
            jnp.concatenate([step, zero], 0) - jnp.concatenate([zero, step], 0)
        )
        return heat + jnp.where(owned, TIME_STEP * vertical, 0.0) - rate * div

    def lane_blocks(x):
        parts = [x[:, b * LANES : (b + 1) * LANES] for b in range(x.shape[1] // LANES)]
        return sum(parts[1:], parts[0])

    def partial_mean(slot, weighted):
        weighted = jnp.sum(weighted, axis=1, keepdims=True)
        whole = jnp.sum(area, axis=1, keepdims=True)
        row_at = lax.broadcasted_iota(jnp.int32, (levels, LANES), 0)
        lane_at = lax.broadcasted_iota(jnp.int32, (levels, LANES), 1)
        row = jnp.sum(jnp.where(row_at == lane_at, weighted, 0.0), axis=0, keepdims=True)
        lane = lax.broadcasted_iota(jnp.int32, (1, LANES), 1)
        row = jnp.where(lane < levels, row, whole)
        mean_send[slot] = jnp.broadcast_to(row, (8, LANES))
        for k in range(1, n):
            to_peer(
                mean_send.at[slot],
                mean_recv.at[slot, k - 1],
                mean_ssem.at[0],
                mean_rsem.at[slot],
                dom_peer(k),
            ).start()

    def mean_row(slot):
        to_peer(
            mean_recv.at[slot],
            mean_recv.at[slot],
            mean_ssem.at[0],
            mean_rsem.at[slot],
            dom_peer(1),
        ).wait_recv()
        total = mean_send[slot]
        for k in range(n - 1):
            total = total + mean_recv[slot, k]
        return total / total[:, levels : levels + 1]

    def as_column(row):
        row_at = lax.broadcasted_iota(jnp.int32, (levels, LANES), 0)
        lane_at = lax.broadcasted_iota(jnp.int32, (levels, LANES), 1)
        return jnp.sum(jnp.where(row_at == lane_at, row[0:1], 0.0), axis=1, keepdims=True)

    with scope("local_0"):
        p_sum, t_sum = local(current, theta)
        loads["q"].wait()
        base = jnp.where(owned, 2.0 * current - q_ref[0], current) + scale * p_sum
        t_base = heat_base(theta, t_sum)
    with scope("base_0"):
        base_s, t_base_s, *turn_s = chosen_of(
            base, t_base, *[-rate * cf[j] for j in range(slabs)]
        )
    share = couple / NS
    with scope("wait_0"):
        t_out_s, ht = relay(0, parted(t_base_s), [parted(x) for x in turn_s])
        base_s = [
            x + share * (new - old)
            for x, new, old in zip(parted(base_s), t_out_s, parted(theta_s))
        ]
        out, hp = relay(1, base_s, weight_s)
        exchange(2, out)
        exchange(STEPS * NS + 1, t_out_s)
        both = jnp.concatenate([ht, hp], axis=0)
    with scope("full_0"):
        theta1 = t_base
        previous, stepped = current, base
        for j in range(slabs):
            y = far(both, j)
            theta1 = theta1 - rate * (cf[j] * fold(y[: 2 * levels]))
            stepped = stepped + (scale * metric[j]) * fold(y[2 * levels :])
        forcing = share * (theta1 - theta)
        current = stepped + forcing

    w_all = to_peer(w_send, w_recv, w_sem.at[0], w_sem.at[1], dom_peer(1))

    def pull(places):
        rows = jnp.concatenate([speed * m for m in metric], axis=1)
        rows = halves(jnp.broadcast_to(rows, (16, slabs * cells)))
        lo, hi = cells + places[0] * hb, cells + (places[-1] + 1) * hb
        w = fold(mm_nt(rows, g[lo:hi, :]))
        for i, u in enumerate(places):
            peer, place = in_from[u]
            w_send[u] = w[0:8, i * hb : (i + 1) * hb]
            to_peer(
                w_send.at[u], w_recv.at[place], w_sem.at[0], w_sem.at[1], peer
            ).start()

    total = STEPS * NS
    for k in range(1, total):
        with scope(f"local_{k}"):
            if k == 1:
                p_sum, t_sum = local(current, theta1)
                t_base = heat_base(theta1, t_sum)
            else:
                p_sum = local(current)
            if k == NS - 1:
                ht = arrived_all(STEPS * NS + 1)
                theta2 = t_base
                for j in range(slabs):
                    theta2 = theta2 - rate * (cf[j] * fold(far(ht, j)))
                t_out[0] = theta2
                t_copy = pltpu.make_async_copy(t_out, t_hold, out_sem.at[0])
                t_copy.start()
            if k == NS:
                forcing = share * (theta2 - theta1)
                partial_mean(0, lane_blocks(current * area))
            base = (
                jnp.where(owned, 2.0 * current - previous, current) + scale * p_sum + forcing
            )
        if k < total - 1:
            with scope(f"base_{k}"):
                (base_s,) = chosen_of(base)
                base_s = parted(base_s)
        else:
            with scope("mean_1"):
                w_all.wait_recv()
                weighted = lane_blocks(base * area)
                for b in range(nb):
                    weighted = weighted + w_recv[b, 0:1] * send[k + 1, b]
                partial_mean(1, weighted)
                first_row = mean_row(0)
                first = as_column(first_row)
        if k in (1, NS):
            with scope(f"pull_{k}"):
                pull(range(nb // 2) if k == 1 else range(nb // 2, nb))
        with scope(f"wait_{k}"):
            if k < total - 1:
                out, hp = relay(k + 1, base_s, weight_s)
                exchange(k + 2, out)
            else:
                hp = arrived_all(k + 1)
        with scope(f"full_{k}"):
            previous, stepped = current, base
            for j in range(slabs):
                stepped = stepped + (scale * metric[j]) * fold(far(hp, j))
            current = stepped

    with scope("tail_send"):
        current = jnp.where(owned, current - first, current)
        pieces = max(stages, 1) * CHUNKS
        width = cells // pieces

        def member_copy(stage, c):
            return to_peer(
                mem_send.at[stage, c],
                mem_recv.at[stage, c],
                mem_ssem.at[0],
                mem_rsem.at[stage, c],
                partner((stage + c) % max(stages, 1)),
            )

        def row_copy(k):
            return to_peer(
                mm_send, mm_recv.at[k - 1], mm_sem.at[0], mm_sem.at[1], member_peer(k)
            )

        for c in range(pieces):
            mem_send[0, c] = current[:, c * width : (c + 1) * width]
            if stages:
                member_copy(0, c).start()
    with scope("tail_mean"):
        last = mean_row(1) - first_row
        mm_send[...] = last
        for k in range(1, members):
            row_copy(k).start()
        column = as_column(last)
        p_out[0] = jnp.where(owned, current - column, current)
        p_copy = pltpu.make_async_copy(p_out, p_hold, out_sem.at[1])
        p_copy.start()
    for s in range(stages - 1):
        with scope(f"tail_stage_{s}"):
            for c in range(pieces):
                member_copy(s, c).wait_recv()
                mem_send[s + 1, c] = mem_send[s, c] + mem_recv[s, c]
                member_copy(s + 1, c).start()
    with scope("tail_rows"):
        summed = last
        if members > 1:
            to_peer(mm_recv, mm_recv, mm_sem.at[0], mm_sem.at[1], member_peer(1)).wait_recv()
            for k in range(members - 1):
                summed = summed + mm_recv[k]
        column = as_column(summed)
    with scope("tail_end"):
        for c in range(pieces):
            cut = slice(c * width, (c + 1) * width)
            field = mem_send[max(stages - 1, 0), c]
            if stages:
                member_copy(stages - 1, c).wait_recv()
                field = field + mem_recv[stages - 1, c]
            e_out[:, cut] = (field - jnp.where(owned[:, cut], column, 0.0)) / members
        e_copy = pltpu.make_async_copy(e_out, e_hold, out_sem.at[2])
        e_copy.start()
    with scope("drain"):
        to_peer(send, recv, send_sem.at[0], recv_sem.at[0, 0], dom_peer(1)).wait_send()
        to_peer(mean_recv, mean_recv, mean_ssem.at[0], mean_rsem.at[0], dom_peer(1)).wait_send()
        w_all.wait_send()
        if stages:
            to_peer(
                mem_send, mem_recv, mem_ssem.at[0], mem_rsem.at[0, 0], partner(0)
            ).wait_send()
        if members > 1:
            to_peer(mm_recv, mm_recv, mm_sem.at[0], mm_sem.at[1], member_peer(1)).wait_send()
        t_copy.wait()
        p_copy.wait()
        e_copy.wait()


def finish(p_hold, t_hold, e_hold, p_out, t_out, e_out, sem):
    copies = [
        pltpu.make_async_copy(src, dst, sem.at[at])
        for at, (src, dst) in enumerate(
            [(p_hold, p_out), (t_hold, t_out), (e_hold, e_out)]
        )
    ]
    for copy in copies:
        copy.start()
    for copy in copies:
        copy.wait()


def solution(mesh):
    n = mesh.shape["dom"]
    members = mesh.shape["member"]

    def per_device(
        acoustic_perturbation,
        prior_acoustic_state,
        thermal_anomaly,
        model_parameters,
        crossing_velocity,
        face_extent,
        face_metric_factor,
        reciprocal_polygon_surface,
        owned_totals,
        export_lists,
        face_neighbour_pair,
        polygon_side_lookup,
    ):
        _, levels, cells = acoustic_perturbation.shape
        edges = face_extent.shape[0]
        slabs = edges // cells
        nb, hb = export_lists.shape[1:]
        halo = nb * hb
        stages = members.bit_length() - 1
        some = max(stages, 1)
        pieces = some * CHUNKS
        slots = STEPS * NS + 2
        hbm = pl.BlockSpec(memory_space=pl.ANY)
        dma = pltpu.SemaphoreType.DMA
        field = pltpu.VMEM((1, levels, cells), F32)
        shapes = (
            jax.ShapeDtypeStruct((1, levels, cells), F32),
            jax.ShapeDtypeStruct((1, levels, cells), F32),
            jax.ShapeDtypeStruct((levels, cells), F32),
        )
        held = pl.pallas_call(
            functools.partial(kernel, n, members),
            out_shape=shapes,
            in_specs=[hbm] * 10,
            out_specs=(hbm, hbm, hbm),
            scratch_shapes=[
                pltpu.SMEM((1, 4), F32),
                field,
                field,
                pltpu.VMEM((levels, cells), F32),
                field,
                field,
                field,
                pltpu.VMEM((levels, edges), F32),
                pltpu.VMEM((1, edges), F32),
                pltpu.VMEM((1, edges), F32),
                pltpu.VMEM((1, cells), F32),
                pltpu.VMEM((1, halo), jnp.int32),
                pltpu.VMEM((2, edges), jnp.int32),
                dma((10,)),
                dma((3,)),
                pltpu.VMEM((1, halo), jnp.int32),
                pltpu.VMEM((cells, halo), F8),
                pltpu.VMEM((cells + halo, edges), F8),
                pltpu.VMEM((halo, slabs * halo), F8),
                pltpu.VMEM((16, edges), F32),
                pltpu.VMEM((8, edges), jnp.int32),
                pltpu.VMEM((16, edges), F32),
                pltpu.VMEM((8, edges), jnp.int32),
                pltpu.VMEM((8, slabs * halo), jnp.int32),
                pltpu.VMEM((slabs, levels, cells), F32),
                pltpu.VMEM((slabs, levels, cells), F32),
                pltpu.VMEM((slots, nb, levels, hb), F32),
                pltpu.VMEM((slots, nb, levels, hb), F32),
                pltpu.VMEM((STEPS, 8, LANES), F32),
                pltpu.VMEM((STEPS, n - 1, 8, LANES), F32),
                pltpu.VMEM((some, pieces, levels, cells // pieces), F32),
                pltpu.VMEM((some, pieces, levels, cells // pieces), F32),
                pltpu.VMEM((8, LANES), F32),
                pltpu.VMEM((max(members - 1, 1), 8, LANES), F32),
                pltpu.VMEM((nb, 8, hb), F32),
                pltpu.VMEM((nb, 8, hb), F32),
                dma((1,)),
                dma((4, nb // GROUP)),
                dma((1,)),
                dma((STEPS,)),
                dma((1,)),
                dma((some, pieces)),
                dma((2,)),
                dma((2,)),
            ],
            compiler_params=pltpu.CompilerParams(
                collective_id=0, has_side_effects=True, vmem_limit_bytes=32 * 1024 * 1024
            ),
        )(
            *[
                pltpu.with_memory_space_constraint(x, pltpu.HBM)
                for x in (
                    model_parameters,
                    acoustic_perturbation,
                    prior_acoustic_state,
                    thermal_anomaly,
                    crossing_velocity,
                    face_extent[None],
                    face_metric_factor[None],
                    reciprocal_polygon_surface[None],
                    export_lists.reshape(1, halo),
                    face_neighbour_pair,
                )
            ],
        )
        return pl.pallas_call(
            finish,
            out_shape=shapes,
            in_specs=[hbm] * 3,
            out_specs=(hbm, hbm, hbm),
            scratch_shapes=[dma((3,))],
            compiler_params=pltpu.CompilerParams(vmem_limit_bytes=1024 * 1024),
        )(*held)

    in_specs = (
        P("member", None, "dom"),
        P("member", None, "dom"),
        P("member", None, "dom"),
        P("member", None),
        P(None, "dom"),
        P("dom"),
        P("dom"),
        P("dom"),
        P("dom"),
        P("dom", None, None),
        P(None, "dom"),
        P(None, "dom"),
    )
    out_specs = (P("member", None, "dom"), P("member", None, "dom"), P(None, "dom"))
    return jax.shard_map(
        per_device, mesh=mesh, in_specs=in_specs, out_specs=out_specs, check_vma=False
    )
```

```python
import functools

import jax
import jax.numpy as jnp
from jax import lax
from jax.experimental import pallas as pl
from jax.experimental.pallas import tpu as pltpu
from jax.sharding import PartitionSpec as P

STEPS = 2
NS = 3
TIME_STEP = 0.25
LANES = 128
CHUNKS = 4
GROUP = 2
MESH = pl.DeviceIdType.MESH
F32 = jnp.float32
BF16 = jnp.bfloat16
F8 = jnp.float8_e4m3fn
I8 = jnp.int8
scope = jax.named_scope


def neighbour_offsets(count):
    return [(b // 2 + 1) * (1 - 2 * (b % 2)) for b in range(count)]


def mm(a, b):
    return jnp.dot(a, b, preferred_element_type=F32)


def mm_nt(a, b):
    return lax.dot_general(a, b, (((1,), (1,)), ((), ())), preferred_element_type=F32)


def halves(x):
    high = x.astype(BF16)
    low = (x - high.astype(F32)).astype(BF16)
    return jnp.concatenate([high, low], axis=0)


def fold(x):
    rows = x.shape[0] // 2
    return x[:rows] + x[rows:]


def one_hot(dst, row_blocks, columns, row_of):
    width = 512 if columns % 512 == 0 else 256 if columns % 256 == 0 else LANES

    def body(b, carry):
        for at in range(0, columns, width):
            cut = slice(at, at + width)
            row = row_of(cut)
            near = jnp.where((row >> 7) == b, row & (LANES - 1), -1)
            near = jnp.broadcast_to(near, (32, width)).astype(I8)
            for s in range(0, LANES, 32):
                rows = (lax.broadcasted_iota(jnp.int32, (32, width), 0) + s).astype(I8)
                dst[pl.ds(pl.multiple_of(b * LANES + s, 32), 32), cut] = jnp.where(
                    rows == near, F8(1), F8(0)
                )
        return carry

    lax.fori_loop(0, row_blocks, body, 0)


def kernel(
    n,
    members,
    par_hbm,
    p_hbm,
    q_hbm,
    t_hbm,
    v_hbm,
    ext_hbm,
    met_hbm,
    inv_hbm,
    exp_hbm,
    fin_hbm,
    p_hold,
    t_hold,
    e_hold,
    par_ref,
    p_out,
    t_out,
    e_out,
    p_ref,
    q_ref,
    t_ref,
    v_ref,
    ext_ref,
    met_ref,
    inv_ref,
    exp_ref,
    fin_ref,
    in_sem,
    out_sem,
    exp_s,
    pick,
    g,
    m3,
    tab,
    itab,
    ej,
    endj,
    ends_s,
    cf,
    ct,
    send,
    recv,
    mean_send,
    mean_recv,
    mem_send,
    mem_recv,
    mm_send,
    mm_recv,
    w_send,
    w_recv,
    en_send,
    en_recv,
    en_sum,
    eh,
    send_sem,
    recv_sem,
    mean_ssem,
    mean_rsem,
    mem_ssem,
    mem_rsem,
    mm_sem,
    w_sem,
    en_sem,
    ready_sem,
    fence_sem,
):
    levels, cells = p_ref.shape[1], p_ref.shape[2]
    slabs = v_ref.shape[1] // cells
    blocks = cells // LANES
    nb, hb = send.shape[1], send.shape[3]
    halo = nb * hb
    me = lax.axis_index("dom")
    mine = lax.axis_index("member")
    stages = members.bit_length() - 1
    groups = nb // GROUP
    lead = nb - GROUP
    spans = [(0, lead), (lead, nb)] if lead else [(0, nb)]
    wide = GROUP * hb

    offsets = neighbour_offsets(nb)
    ahead = [o for o in sorted(offsets, reverse=True) if o > 0]
    behind = [o for o in sorted(offsets, reverse=True) if o < 0]
    out_offsets = behind[1:] + behind[:1] + ahead
    in_offsets = behind + ahead[-1:] + ahead[:-1]
    out_blocks = [offsets.index(o) for o in out_offsets]
    in_blocks = [offsets.index(o) for o in in_offsets]
    half = (n + 1) // 2
    upper = me // half

    def turned(block):
        return block + upper * (1 - 2 * (block % 2))

    def meet(offset, block, order):
        peer = lax.rem(me + offset * (1 - 2 * upper) + n * nb, n)
        other = peer // half
        differ = upper + other - 2 * upper * other
        here, there = order.index(block), order.index(block + 1 - 2 * (block % 2))
        return {"dom": peer}, here + differ * (there - here)

    out_to = [meet(o, b, in_blocks) for o, b in zip(out_offsets, out_blocks)]
    in_from = [meet(-o, b, out_blocks) for o, b in zip(in_offsets, in_blocks)]

    def dom_peer(k):
        return {"dom": lax.rem(me + (k % n), n)}

    def member_peer(k):
        return {"member": lax.rem(mine + (k % members), members)}

    def partner(stage):
        bit = 1 << stage
        return {"member": mine + bit - 2 * bit * lax.rem(mine // bit, 2)}

    with scope("start"):
        barrier = pltpu.get_barrier_semaphore()
        for k in range(1, n):
            pl.semaphore_signal(barrier, inc=1, device_id=dom_peer(k), device_id_type=MESH)
        for k in range(1, members):
            pl.semaphore_signal(barrier, inc=1, device_id=member_peer(k), device_id_type=MESH)
        loads = {}
        for at, (name, src, dst) in enumerate(
            [
                ("exp", exp_hbm, exp_ref),
                ("t", t_hbm, t_ref),
                ("p", p_hbm, p_ref),
                ("fin", fin_hbm, fin_ref),
                ("par", par_hbm, par_ref),
                ("met", met_hbm, met_ref),
                ("inv", inv_hbm, inv_ref),
                ("ext", ext_hbm, ext_ref),
                ("v", v_hbm, v_ref),
                ("q", q_hbm, q_ref),
            ]
        ):
            loads[name] = pltpu.make_async_copy(src, dst, in_sem.at[at])
            loads[name].start()


    def to_peer(src, dst, send_sem, recv_sem, peer):
        return pltpu.make_async_remote_copy(
            src_ref=src,
            dst_ref=dst,
            send_sem=send_sem,
            recv_sem=recv_sem,
            device_id=peer,
            device_id_type=MESH,
        )

    rows_of = [2] + [k % 2 for k in range(STEPS * NS)] + [3]

    def give(slot, part, x):
        for t in range(part * GROUP, (part + 1) * GROUP):
            peer, place = out_to[t]
            at = t % GROUP * hb
            send[slot, t] = x[:, at : at + hb]
            to_peer(
                send.at[slot, t],
                recv.at[slot, place],
                send_sem.at[0],
                recv_sem.at[rows_of[slot], place // lead if lead else 0],
                peer,
            ).start()

    def fence():
        pl.semaphore_signal(fence_sem, 1)
        pl.semaphore_wait(fence_sem, 1)

    def exchange(slot, parts):
        for part, x in enumerate(parts):
            give(slot, part, x)

    def arrived(slot, group):
        lo, hi = spans[group]
        to_peer(
            send.at[slot, lo:hi],
            recv.at[slot, lo:hi],
            send_sem.at[0],
            recv_sem.at[rows_of[slot], group],
            dom_peer(1),
        ).wait_recv()
        return halves(jnp.concatenate([recv[slot, u] for u in range(lo, hi)], axis=1))

    def parted(x):
        return [x[:, at : at + wide] for at in range(0, halo, wide)]

    def chosen_of(*fields):
        y = mm(jnp.concatenate([halves(x) for x in fields], axis=0), pick[...])
        return [fold(y[2 * levels * i : 2 * levels * (i + 1)]) for i in range(len(fields))]

    with scope("pick_build"):
        loads["exp"].wait()
        for t, block in enumerate(out_blocks):
            at = pl.multiple_of(turned(block) * hb, hb)
            exp_s[0:1, t * hb : (t + 1) * hb] = exp_ref[0:1, pl.ds(at, hb)]
        one_hot(pick, blocks, halo, lambda cut: exp_s[0:1, cut])
    with scope("pick0"):
        loads["t"].wait()
        loads["p"].wait()
        current = p_ref[0]
        theta = t_ref[0]
        theta_s, current_s = chosen_of(theta, current)

    with scope("tables"):
        loads["fin"].wait()
        loads["met"].wait()
        loads["inv"].wait()
        loads["ext"].wait()
        loads["par"].wait()
        speed = par_ref[0, 0]
        kappa = 0.5 * par_ref[0, 1]
        mixing = 0.6 * par_ref[0, 2]
        couple = par_ref[0, 3]
        tab[0:8, :] = jnp.broadcast_to(met_ref[...], (8, slabs * cells))
        tab[8:16, :] = jnp.broadcast_to(ext_ref[...], (8, slabs * cells))
        ends = fin_ref[1:2, :]
        block = (ends >> 7) - blocks
        block = block + upper * (1 - 2 * (block & 1))
        place = block
        for b in range(nb):
            place = jnp.where(block == b, in_blocks.index(b), place)
        inner = (ends >= cells) & (ends < cells + halo)
        ends = jnp.where(inner, cells + place * hb + (ends & (hb - 1)), ends)
        itab[...] = jnp.broadcast_to(ends, (8, slabs * cells))

        def slab(ref, rows, b, j):
            at = slabs * lax.broadcasted_iota(jnp.int32, (rows, LANES), 1) + j
            block, lane = at >> 7, at & (LANES - 1)
            out = None
            for s in range(slabs):
                lo = (slabs * b + s) * LANES
                y = jnp.take_along_axis(
                    ref[0:rows, lo : lo + LANES], lane, axis=1, mode="promise_in_bounds"
                )
                out = y if out is None else jnp.where(block == s, y, out)
            return out

        for b in range(blocks):
            for j in range(slabs):
                lo = j * cells + b * LANES
                ej[:, lo : lo + LANES] = slab(tab, 16, b, j)
                endj[:, lo : lo + LANES] = slab(itab, 8, b, j)
        inverse = inv_ref[...]
        owned = endj[0:1, :cells] < cells + halo
        area = jnp.where(owned, 1.0 / inverse, 0.0)
        scale = jnp.where(owned, speed * inverse, 0.0)
        rate = jnp.where(owned, TIME_STEP * inverse, 0.0)
    cuts = [slice(j * cells, (j + 1) * cells) for j in range(slabs)]
    metric = [ej[0:1, cut] for cut in cuts]
    extent = [ej[8:9, cut] for cut in cuts]

    with scope("bar_wait"):
        pl.semaphore_wait(barrier, n - 1 + members - 1)
    with scope("send0"):
        exchange(0, parted(theta_s))
        exchange(1, parted(current_s))

        for k in range(1, members):
            pl.semaphore_signal(ready_sem, inc=1, device_id=member_peer(k), device_id_type=MESH)

    with scope("g_build"):
        one_hot(g, (cells + halo) // LANES, slabs * cells, lambda cut: endj[0:1, cut])
    with scope("coef"):
        loads["v"].wait()
        for j in range(slabs):
            for b in range(blocks):
                lanes = slice(b * LANES, (b + 1) * LANES)
                wind = slab(v_ref, levels, b, j)
                down = extent[j][:, lanes] * (0.5 * wind - (0.5 * jnp.abs(wind) + kappa))
                cf[j, :, lanes] = down
                ct[j, :, lanes] = extent[j][:, lanes] * wind - down
    with scope("m3_build"):
        rows = [endj[0:1, cut].astype(F32) for cut in cuts] + [scale * m for m in metric]
        rows = jnp.concatenate(rows + [jnp.zeros((16 - 2 * slabs, cells), F32)], axis=0)
        y = fold(mm(halves(rows), pick[...]))
        for j in range(slabs):
            for at, part in enumerate(parted(y[j : j + 1])):
                lo = (at * slabs + j) * wide
                ends_s[0:1, lo : lo + wide] = part.astype(jnp.int32) - cells
        weight_s = [parted(y[slabs + j : slabs + j + 1]) for j in range(slabs)]
        one_hot(m3, nb, slabs * halo, lambda cut: ends_s[0:1, cut])

    def local(pressure, heat=None):
        lhs = [halves(pressure)] + ([] if heat is None else [halves(heat)])
        lhs = jnp.concatenate(lhs, axis=0)
        p_flux, t_flux = [], []
        for j in range(slabs):
            y = mm(lhs, g[:cells, cuts[j]])
            p_flux.append(metric[j] * (fold(y[: 2 * levels]) - pressure))
            if heat is not None:
                t_flux.append(cf[j] * fold(y[2 * levels :]) + ct[j] * heat)
        lhs = [halves(jnp.concatenate(p_flux, axis=1))]
        if heat is not None:
            lhs.append(halves(jnp.concatenate(t_flux, axis=1)))
        y = mm_nt(jnp.concatenate(lhs, axis=0), g[:cells, :])
        p_sum = sum(p_flux[1:], p_flux[0]) - fold(y[: 2 * levels])
        if heat is None:
            return p_sum
        return p_sum, sum(t_flux[1:], t_flux[0]) - fold(y[2 * levels :])

    def far(x, j):
        return mm(x, g[cells:, cuts[j]])

    def relay(slot, parts, weights, to=None):
        held = []
        parts = list(parts)
        for group, (lo, hi) in enumerate(spans):
            x = arrived(slot, group)
            held.append(x)
            found = []
            for part in range(groups):
                at = part * slabs * wide
                found.append(mm(x, m3[lo * hb : hi * hb, at : at + slabs * wide]))
            for part, y in enumerate(found):
                for j in range(slabs):
                    parts[part] = parts[part] + weights[j][part] * fold(
                        y[:, j * wide : (j + 1) * wide]
                    )
                if to is not None and hi == nb:
                    give(to, part, parts[part])
        return parts, jnp.concatenate(held, axis=1)

    def arrived_all(slot):
        return jnp.concatenate([arrived(slot, i) for i in range(len(spans))], axis=1)

    def heat_base(heat, div):
        step = heat[1:] - heat[:-1]
        zero = jnp.zeros((1, cells), F32)
        vertical = mixing * (
            jnp.concatenate([step, zero], 0) - jnp.concatenate([zero, step], 0)
        )
        return heat + jnp.where(owned, TIME_STEP * vertical, 0.0) - rate * div

    def lane_blocks(x):
        parts = [x[:, b * LANES : (b + 1) * LANES] for b in range(x.shape[1] // LANES)]
        return sum(parts[1:], parts[0])

    def partial_mean(slot, weighted):
        weighted = jnp.sum(weighted, axis=1, keepdims=True)
        whole = jnp.sum(area, axis=1, keepdims=True)
        row_at = lax.broadcasted_iota(jnp.int32, (levels, LANES), 0)
        lane_at = lax.broadcasted_iota(jnp.int32, (levels, LANES), 1)
        row = jnp.sum(jnp.where(row_at == lane_at, weighted, 0.0), axis=0, keepdims=True)
        lane = lax.broadcasted_iota(jnp.int32, (1, LANES), 1)
        row = jnp.where(lane < levels, row, whole)
        mean_send[slot] = jnp.broadcast_to(row, (8, LANES))
        for k in range(1, n):
            to_peer(
                mean_send.at[slot],
                mean_recv.at[slot, k - 1],
                mean_ssem.at[0],
                mean_rsem.at[slot],
                dom_peer(k),
            ).start()
        return row

    def mean_row(slot):
        to_peer(
            mean_recv.at[slot],
            mean_recv.at[slot],
            mean_ssem.at[0],
            mean_rsem.at[slot],
            dom_peer(1),
        ).wait_recv()
        total = mean_send[slot]
        for k in range(n - 1):
            total = total + mean_recv[slot, k]
        return total / total[:, levels : levels + 1]

    def as_column(row):
        row_at = lax.broadcasted_iota(jnp.int32, (levels, LANES), 0)
        lane_at = lax.broadcasted_iota(jnp.int32, (levels, LANES), 1)
        return jnp.sum(jnp.where(row_at == lane_at, row[0:1], 0.0), axis=1, keepdims=True)

    with scope("local_0"):
        p_sum, t_sum = local(current, theta)
        loads["q"].wait()
        base = jnp.where(owned, 2.0 * current - q_ref[0], current) + scale * p_sum
        t_base = heat_base(theta, t_sum)
    with scope("base_0"):
        base_s, t_base_s, *turn_s = chosen_of(
            base, t_base, *[-rate * cf[j] for j in range(slabs)]
        )
    share = couple / NS
    with scope("wait_0"):
        t_out_s, ht = relay(0, parted(t_base_s), [parted(x) for x in turn_s])
        base_s = [
            x + share * (new - old)
            for x, new, old in zip(parted(base_s), t_out_s, parted(theta_s))
        ]
        _, hp = relay(1, base_s, weight_s, 2)
        exchange(STEPS * NS + 1, t_out_s)
        fence()
        both = jnp.concatenate([ht, hp], axis=0)
    with scope("full_0"):
        theta1 = t_base
        previous, stepped = current, base
        for j in range(slabs):
            y = far(both, j)
            theta1 = theta1 - rate * (cf[j] * fold(y[: 2 * levels]))
            stepped = stepped + (scale * metric[j]) * fold(y[2 * levels :])
        forcing = share * (theta1 - theta)
        current = stepped + forcing

    w_all = to_peer(w_send, w_recv, w_sem.at[0], w_sem.at[1], dom_peer(1))

    def pull(places):
        rows = jnp.concatenate([speed * m for m in metric], axis=1)
        rows = halves(jnp.broadcast_to(rows, (16, slabs * cells)))
        lo, hi = cells + places[0] * hb, cells + (places[-1] + 1) * hb
        w = fold(mm_nt(rows, g[lo:hi, :]))
        for i, u in enumerate(places):
            peer, place = in_from[u]
            w_send[u] = w[0:8, i * hb : (i + 1) * hb]
            to_peer(
                w_send.at[u], w_recv.at[place], w_sem.at[0], w_sem.at[1], peer
            ).start()

    layer = levels // members
    en_all = to_peer(en_recv, en_recv, en_sem.at[0], en_sem.at[1], member_peer(1))
    eh_all = to_peer(eh, eh, en_sem.at[2], en_sem.at[3], dom_peer(1))

    def gather_exports(parts):
        for t in range(nb):
            at = t % GROUP * hb
            x = speed * parts[t // GROUP][:, at : at + hb]
            for m in range(members):
                en_send[m, t] = x[m * layer : (m + 1) * layer]
        for k in range(1, members):
            to = lax.rem(mine + k, members)
            to_peer(
                en_send.at[to], en_recv.at[k - 1], en_sem.at[0], en_sem.at[1], {"member": to}
            ).start()

    def spread_exports():
        if members > 1:
            en_all.wait_recv()
        summed = en_send[mine]
        for k in range(members - 1):
            summed = summed + en_recv[k]
        en_sum[...] = summed
        rows = pl.ds(pl.multiple_of(mine * layer, layer), layer)
        for t, (peer, place) in enumerate(out_to):
            for k in range(members):
                to_peer(
                    en_sum.at[t],
                    eh.at[place, rows],
                    en_sem.at[2],
                    en_sem.at[3],
                    {**peer, "member": lax.rem(mine + k, members)},
                ).start()

    some = max(stages, 1)
    pieces = some * CHUNKS
    width = cells // pieces

    def member_copy(stage, c):
        return to_peer(
            mem_send.at[stage, c],
            mem_recv.at[stage, c],
            mem_ssem.at[0],
            mem_rsem.at[stage, c // some],
            partner((stage + c) % some),
        )

    def chunk_wait(stage, group):
        at = slice(group * some, (group + 1) * some)
        to_peer(
            mem_send.at[stage, at],
            mem_recv.at[stage, at],
            mem_ssem.at[0],
            mem_rsem.at[stage, group],
            partner(0),
        ).wait_recv()

    total = STEPS * NS
    for k in range(1, total):
        if k == total - 2 and members > 1:
            pl.semaphore_wait(ready_sem, members - 1)
        with scope(f"local_{k}"):
            if k == 1:
                p_sum, t_sum = local(current, theta1)
                t_base = heat_base(theta1, t_sum)
            else:
                p_sum = local(current)
            if k == NS:
                forcing = share * (theta2 - theta1)
                partial_mean(0, lane_blocks(current * area))
            base = (
                jnp.where(owned, 2.0 * current - previous, current) + scale * p_sum + forcing
            )
        if k < total - 1:
            with scope(f"base_{k}"):
                (base_s,) = chosen_of(base)
                base_s = parted(base_s)
        else:
            with scope("bulk"):
                for c in range(pieces):
                    mem_send[0, c] = base[:, c * width : (c + 1) * width]
                    if stages:
                        member_copy(0, c).start()
            with scope("mean_1"):
                w_all.wait_recv()
                weighted = lane_blocks(base * area)
                for b in range(nb):
                    weighted = weighted + w_recv[b, 0:1] * send[k + 1, b]
                mm_send[...] = partial_mean(1, weighted)
                for m in range(1, members):
                    for d in range(n):
                        to_peer(
                            mm_send,
                            mm_recv.at[m - 1, d],
                            mm_sem.at[0],
                            mm_sem.at[1],
                            {**dom_peer(d), **member_peer(m)},
                        ).start()
                first_row = mean_row(0)
                first = as_column(first_row)
            with scope("spread"):
                spread_exports()
        if k == NS - 1:
            with scope("heat_2"):
                ht = arrived_all(STEPS * NS + 1)
                theta2 = t_base
                for j in range(slabs):
                    theta2 = theta2 - rate * (cf[j] * fold(far(ht, j)))
                t_out[0] = theta2
                t_copy = pltpu.make_async_copy(t_out, t_hold, out_sem.at[0])
                t_copy.start()
        if k in (1, NS):
            with scope(f"pull_{k}"):
                pull(range(nb // 2) if k == 1 else range(nb // 2, nb))
        with scope(f"wait_{k}"):
            if k < total - 1:
                out, hp = relay(k + 1, base_s, weight_s, k + 2)
                if k == total - 2:
                    gather_exports(out)
                fence()
            else:
                hp = arrived_all(k + 1)
        with scope(f"full_{k}"):
            previous, stepped = current, base
            for j in range(slabs):
                stepped = stepped + (scale * metric[j]) * fold(far(hp, j))
            current = stepped

    for s in range(stages - 1):
        with scope(f"tail_stage_{s}"):
            for c in range(pieces):
                if c % some == 0:
                    chunk_wait(s, c // some)
                mem_send[s + 1, c] = mem_send[s, c] + mem_recv[s, c]
                member_copy(s + 1, c).start()
    with scope("tail_mean"):
        current = jnp.where(owned, current - first, current)
        last = mean_row(1) - first_row
        p_out[0] = jnp.where(owned, current - as_column(last), current)
        p_copy = pltpu.make_async_copy(p_out, p_hold, out_sem.at[1])
        p_copy.start()
    with scope("tail_far"):
        eh_all.wait_recv()
        x = halves(jnp.concatenate([eh[u] for u in range(nb)], axis=1))
        field = jnp.zeros((levels, cells), F32)
        for j in range(slabs):
            field = field + jnp.where(owned, inverse * metric[j], 0.0) * fold(far(x, j))
    with scope("tail_rows"):
        summed = (first_row + last)[0:1]
        if members > 1:
            to_peer(mm_recv, mm_recv, mm_sem.at[0], mm_sem.at[1], member_peer(1)).wait_recv()
            for m in range(members - 1):
                row = mm_recv[m, 0]
                for d in range(1, n):
                    row = row + mm_recv[m, d]
                summed = summed + row / row[:, levels : levels + 1]
        field = field - jnp.where(owned, as_column(summed), 0.0)
    with scope("tail_end"):
        for c in range(pieces):
            cut = slice(c * width, (c + 1) * width)
            x = mem_send[some - 1, c]
            if stages:
                if c % some == 0:
                    chunk_wait(stages - 1, c // some)
                x = x + mem_recv[stages - 1, c]
            e_out[:, cut] = (x + field[:, cut]) / members
        e_copy = pltpu.make_async_copy(e_out, e_hold, out_sem.at[2])
        e_copy.start()
    with scope("drain"):
        to_peer(send, recv, send_sem.at[0], recv_sem.at[0, 0], dom_peer(1)).wait_send()
        to_peer(mean_recv, mean_recv, mean_ssem.at[0], mean_rsem.at[0], dom_peer(1)).wait_send()
        w_all.wait_send()
        if members > 1:
            en_all.wait_send()
        eh_all.wait_send()
        if stages:
            to_peer(
                mem_send, mem_recv, mem_ssem.at[0], mem_rsem.at[0, 0], partner(0)
            ).wait_send()
        if members > 1:
            to_peer(mm_recv, mm_recv, mm_sem.at[0], mm_sem.at[1], member_peer(1)).wait_send()
        t_copy.wait()
        p_copy.wait()
        e_copy.wait()


def finish(p_hold, t_hold, e_hold, p_out, t_out, e_out, sem):
    copies = [
        pltpu.make_async_copy(src, dst, sem.at[at])
        for at, (src, dst) in enumerate(
            [(p_hold, p_out), (t_hold, t_out), (e_hold, e_out)]
        )
    ]
    for copy in copies:
        copy.start()
    for copy in copies:
        copy.wait()


def solution(mesh):
    n = mesh.shape["dom"]
    members = mesh.shape["member"]

    def per_device(
        acoustic_perturbation,
        prior_acoustic_state,
        thermal_anomaly,
        model_parameters,
        crossing_velocity,
        face_extent,
        face_metric_factor,
        reciprocal_polygon_surface,
        owned_totals,
        export_lists,
        face_neighbour_pair,
        polygon_side_lookup,
    ):
        _, levels, cells = acoustic_perturbation.shape
        edges = face_extent.shape[0]
        slabs = edges // cells
        nb, hb = export_lists.shape[1:]
        halo = nb * hb
        stages = members.bit_length() - 1
        some = max(stages, 1)
        pieces = some * CHUNKS
        slots = STEPS * NS + 2
        hbm = pl.BlockSpec(memory_space=pl.ANY)
        dma = pltpu.SemaphoreType.DMA
        field = pltpu.VMEM((1, levels, cells), F32)
        shapes = (
            jax.ShapeDtypeStruct((1, levels, cells), F32),
            jax.ShapeDtypeStruct((1, levels, cells), F32),
            jax.ShapeDtypeStruct((levels, cells), F32),
        )
        held = pl.pallas_call(
            functools.partial(kernel, n, members),
            out_shape=shapes,
            in_specs=[hbm] * 10,
            out_specs=(hbm, hbm, hbm),
            scratch_shapes=[
                pltpu.SMEM((1, 4), F32),
                field,
                field,
                pltpu.VMEM((levels, cells), F32),
                field,
                field,
                field,
                pltpu.VMEM((levels, edges), F32),
                pltpu.VMEM((1, edges), F32),
                pltpu.VMEM((1, edges), F32),
                pltpu.VMEM((1, cells), F32),
                pltpu.VMEM((1, halo), jnp.int32),
                pltpu.VMEM((2, edges), jnp.int32),
                dma((10,)),
                dma((3,)),
                pltpu.VMEM((1, halo), jnp.int32),
                pltpu.VMEM((cells, halo), F8),
                pltpu.VMEM((cells + halo, edges), F8),
                pltpu.VMEM((halo, slabs * halo), F8),
                pltpu.VMEM((16, edges), F32),
                pltpu.VMEM((8, edges), jnp.int32),
                pltpu.VMEM((16, edges), F32),
                pltpu.VMEM((8, edges), jnp.int32),
                pltpu.VMEM((8, slabs * halo), jnp.int32),
                pltpu.VMEM((slabs, levels, cells), F32),
                pltpu.VMEM((slabs, levels, cells), F32),
                pltpu.VMEM((slots, nb, levels, hb), F32),
                pltpu.VMEM((slots, nb, levels, hb), F32),
                pltpu.VMEM((STEPS, 8, LANES), F32),
                pltpu.VMEM((STEPS, n - 1, 8, LANES), F32),
                pltpu.VMEM((some, pieces, levels, cells // pieces), F32),
                pltpu.VMEM((some, pieces, levels, cells // pieces), F32),
                pltpu.VMEM((1, LANES), F32),
                pltpu.VMEM((max(members - 1, 1), n, 1, LANES), F32),
                pltpu.VMEM((nb, 8, hb), F32),
                pltpu.VMEM((nb, 8, hb), F32),
                pltpu.VMEM((members, nb, levels // members, hb), F32),
                pltpu.VMEM((max(members - 1, 1), nb, levels // members, hb), F32),
                pltpu.VMEM((nb, levels // members, hb), F32),
                pltpu.VMEM((nb, levels, hb), F32),
                dma((1,)),
                dma((4, 2)),
                dma((1,)),
                dma((STEPS,)),
                dma((1,)),
                dma((some, CHUNKS)),
                dma((2,)),
                dma((2,)),
                dma((4,)),
                pltpu.SemaphoreType.REGULAR,
                pltpu.SemaphoreType.REGULAR,
            ],
            compiler_params=pltpu.CompilerParams(
                collective_id=0, has_side_effects=True, vmem_limit_bytes=32 * 1024 * 1024
            ),
        )(
            *[
                pltpu.with_memory_space_constraint(x, pltpu.HBM)
                for x in (
                    model_parameters,
                    acoustic_perturbation,
                    prior_acoustic_state,
                    thermal_anomaly,
                    crossing_velocity,
                    face_extent[None],
                    face_metric_factor[None],
                    reciprocal_polygon_surface[None],
                    export_lists.reshape(1, halo),
                    face_neighbour_pair,
                )
            ],
        )
        return pl.pallas_call(
            finish,
            out_shape=shapes,
            in_specs=[hbm] * 3,
            out_specs=(hbm, hbm, hbm),
            scratch_shapes=[dma((3,))],
            compiler_params=pltpu.CompilerParams(vmem_limit_bytes=1024 * 1024),
        )(*held)

    in_specs = (
        P("member", None, "dom"),
        P("member", None, "dom"),
        P("member", None, "dom"),
        P("member", None),
        P(None, "dom"),
        P("dom"),
        P("dom"),
        P("dom"),
        P("dom"),
        P("dom", None, None),
        P(None, "dom"),
        P(None, "dom"),
    )
    out_specs = (P("member", None, "dom"), P("member", None, "dom"), P(None, "dom"))
    return jax.shard_map(
        per_device, mesh=mesh, in_specs=in_specs, out_specs=out_specs, check_vma=False
    )
```

```python
import functools

import jax
import jax.numpy as jnp
from jax import lax
from jax.experimental import pallas as pl
from jax.experimental.pallas import tpu as pltpu
from jax.sharding import PartitionSpec as P

STEPS = 2
NS = 3
TIME_STEP = 0.25
LANES = 128
CHUNKS = 4
GROUP = 2
MESH = pl.DeviceIdType.MESH
F32 = jnp.float32
BF16 = jnp.bfloat16
F8 = jnp.float8_e4m3fn
I8 = jnp.int8
scope = jax.named_scope


def neighbour_offsets(count):
    return [(b // 2 + 1) * (1 - 2 * (b % 2)) for b in range(count)]


def mm(a, b):
    return jnp.dot(a, b, preferred_element_type=F32)


def mm_nt(a, b):
    return lax.dot_general(a, b, (((1,), (1,)), ((), ())), preferred_element_type=F32)


def halves(x):
    high = x.astype(BF16)
    low = (x - high.astype(F32)).astype(BF16)
    return jnp.concatenate([high, low], axis=0)


def fold(x):
    rows = x.shape[0] // 2
    return x[:rows] + x[rows:]


def one_hot(dst, row_blocks, columns, row_of):
    width = 512 if columns % 512 == 0 else 256 if columns % 256 == 0 else LANES

    def body(b, carry):
        for at in range(0, columns, width):
            cut = slice(at, at + width)
            row = row_of(cut)
            near = jnp.where((row >> 7) == b, row & (LANES - 1), -1)
            near = jnp.broadcast_to(near, (32, width)).astype(I8)
            for s in range(0, LANES, 32):
                rows = (lax.broadcasted_iota(jnp.int32, (32, width), 0) + s).astype(I8)
                dst[pl.ds(pl.multiple_of(b * LANES + s, 32), 32), cut] = jnp.where(
                    rows == near, F8(1), F8(0)
                )
        return carry

    lax.fori_loop(0, row_blocks, body, 0)


def kernel(
    n,
    members,
    par_hbm,
    p_hbm,
    q_hbm,
    t_hbm,
    v_hbm,
    ext_hbm,
    met_hbm,
    inv_hbm,
    exp_hbm,
    fin_hbm,
    p_hold,
    t_hold,
    e_hold,
    par_ref,
    p_out,
    t_out,
    e_out,
    p_ref,
    q_ref,
    t_ref,
    v_ref,
    ext_ref,
    met_ref,
    inv_ref,
    exp_ref,
    fin_ref,
    in_sem,
    out_sem,
    exp_s,
    pick,
    g,
    m3,
    tab,
    itab,
    ej,
    endj,
    ends_s,
    cf,
    ct,
    send,
    recv,
    mean_send,
    mean_recv,
    mem_send,
    mem_recv,
    mm_send,
    mm_recv,
    w_send,
    w_recv,
    en_send,
    en_recv,
    en_sum,
    eh,
    send_sem,
    recv_sem,
    mean_ssem,
    mean_rsem,
    mem_ssem,
    mem_rsem,
    mm_sem,
    w_sem,
    en_sem,
    ready_sem,
    fence_sem,
):
    levels, cells = p_ref.shape[1], p_ref.shape[2]
    slabs = v_ref.shape[1] // cells
    blocks = cells // LANES
    nb, hb = send.shape[1], send.shape[3]
    halo = nb * hb
    me = lax.axis_index("dom")
    mine = lax.axis_index("member")
    stages = members.bit_length() - 1
    groups = nb // GROUP
    lead = nb - GROUP
    spans = [(0, lead), (lead, nb)] if lead else [(0, nb)]
    wide = GROUP * hb

    offsets = neighbour_offsets(nb)
    ahead = [o for o in sorted(offsets, reverse=True) if o > 0]
    behind = [o for o in sorted(offsets, reverse=True) if o < 0]
    out_offsets = behind[1:] + behind[:1] + ahead
    in_offsets = behind + ahead[-1:] + ahead[:-1]
    out_blocks = [offsets.index(o) for o in out_offsets]
    in_blocks = [offsets.index(o) for o in in_offsets]
    half = (n + 1) // 2
    upper = me // half

    def turned(block):
        return block + upper * (1 - 2 * (block % 2))

    def meet(offset, block, order):
        peer = lax.rem(me + offset * (1 - 2 * upper) + n * nb, n)
        other = peer // half
        differ = upper + other - 2 * upper * other
        here, there = order.index(block), order.index(block + 1 - 2 * (block % 2))
        return {"dom": peer}, here + differ * (there - here)

    out_to = [meet(o, b, in_blocks) for o, b in zip(out_offsets, out_blocks)]
    in_from = [meet(-o, b, out_blocks) for o, b in zip(in_offsets, in_blocks)]

    def dom_peer(k):
        return {"dom": lax.rem(me + (k % n), n)}

    def member_peer(k):
        return {"member": lax.rem(mine + (k % members), members)}

    def partner(stage):
        bit = 1 << stage
        return {"member": mine + bit - 2 * bit * lax.rem(mine // bit, 2)}

    with scope("start"):
        barrier = pltpu.get_barrier_semaphore()
        for k in range(1, n):
            pl.semaphore_signal(barrier, inc=1, device_id=dom_peer(k), device_id_type=MESH)
        for k in range(1, members):
            pl.semaphore_signal(barrier, inc=1, device_id=member_peer(k), device_id_type=MESH)
        loads = {}
        for at, (name, src, dst) in enumerate(
            [
                ("exp", exp_hbm, exp_ref),
                ("t", t_hbm, t_ref),
                ("p", p_hbm, p_ref),
                ("fin", fin_hbm, fin_ref),
                ("par", par_hbm, par_ref),
                ("met", met_hbm, met_ref),
                ("inv", inv_hbm, inv_ref),
                ("ext", ext_hbm, ext_ref),
                ("v", v_hbm, v_ref),
                ("q", q_hbm, q_ref),
            ]
        ):
            loads[name] = pltpu.make_async_copy(src, dst, in_sem.at[at])
            loads[name].start()


    def to_peer(src, dst, send_sem, recv_sem, peer):
        return pltpu.make_async_remote_copy(
            src_ref=src,
            dst_ref=dst,
            send_sem=send_sem,
            recv_sem=recv_sem,
            device_id=peer,
            device_id_type=MESH,
        )

    rows_of = [2] + [k % 2 for k in range(STEPS * NS)] + [3]

    def give(slot, part, x):
        for t in range(part * GROUP, (part + 1) * GROUP):
            peer, place = out_to[t]
            at = t % GROUP * hb
            send[slot, t] = x[:, at : at + hb]
            to_peer(
                send.at[slot, t],
                recv.at[slot, place],
                send_sem.at[0],
                recv_sem.at[rows_of[slot], place // lead if lead else 0],
                peer,
            ).start()

    def fence():
        pl.semaphore_signal(fence_sem, 1)
        pl.semaphore_wait(fence_sem, 1)

    def exchange(slot, parts):
        for part, x in enumerate(parts):
            give(slot, part, x)

    def arrived(slot, group):
        lo, hi = spans[group]
        to_peer(
            send.at[slot, lo:hi],
            recv.at[slot, lo:hi],
            send_sem.at[0],
            recv_sem.at[rows_of[slot], group],
            dom_peer(1),
        ).wait_recv()
        return halves(jnp.concatenate([recv[slot, u] for u in range(lo, hi)], axis=1))

    def parted(x):
        return [x[:, at : at + wide] for at in range(0, halo, wide)]

    def chosen_of(*fields):
        y = mm(jnp.concatenate([halves(x) for x in fields], axis=0), pick[...])
        return [fold(y[2 * levels * i : 2 * levels * (i + 1)]) for i in range(len(fields))]

    with scope("pick_build"):
        loads["exp"].wait()
        for t, block in enumerate(out_blocks):
            at = pl.multiple_of(turned(block) * hb, hb)
            exp_s[0:1, t * hb : (t + 1) * hb] = exp_ref[0:1, pl.ds(at, hb)]
        one_hot(pick, blocks, halo, lambda cut: exp_s[0:1, cut])
    with scope("pick0"):
        loads["t"].wait()
        loads["p"].wait()
        current = p_ref[0]
        theta = t_ref[0]
        (theta_s,) = chosen_of(theta)

    with scope("tables"):
        loads["fin"].wait()
        loads["met"].wait()
        loads["inv"].wait()
        loads["ext"].wait()
        loads["par"].wait()
        speed = par_ref[0, 0]
        kappa = 0.5 * par_ref[0, 1]
        mixing = 0.6 * par_ref[0, 2]
        couple = par_ref[0, 3]
        tab[0:8, :] = jnp.broadcast_to(met_ref[...], (8, slabs * cells))
        tab[8:16, :] = jnp.broadcast_to(ext_ref[...], (8, slabs * cells))
        ends = fin_ref[1:2, :]
        block = (ends >> 7) - blocks
        block = block + upper * (1 - 2 * (block & 1))
        place = block
        for b in range(nb):
            place = jnp.where(block == b, in_blocks.index(b), place)
        inner = (ends >= cells) & (ends < cells + halo)
        ends = jnp.where(inner, cells + place * hb + (ends & (hb - 1)), ends)
        itab[...] = jnp.broadcast_to(ends, (8, slabs * cells))

        def slab(ref, rows, b, j):
            at = slabs * lax.broadcasted_iota(jnp.int32, (rows, LANES), 1) + j
            block, lane = at >> 7, at & (LANES - 1)
            out = None
            for s in range(slabs):
                lo = (slabs * b + s) * LANES
                y = jnp.take_along_axis(
                    ref[0:rows, lo : lo + LANES], lane, axis=1, mode="promise_in_bounds"
                )
                out = y if out is None else jnp.where(block == s, y, out)
            return out

        for b in range(blocks):
            for j in range(slabs):
                lo = j * cells + b * LANES
                ej[:, lo : lo + LANES] = slab(tab, 16, b, j)
                endj[:, lo : lo + LANES] = slab(itab, 8, b, j)
        inverse = inv_ref[...]
        owned = endj[0:1, :cells] < cells + halo
        area = jnp.where(owned, 1.0 / inverse, 0.0)
        scale = jnp.where(owned, speed * inverse, 0.0)
        rate = jnp.where(owned, TIME_STEP * inverse, 0.0)
    cuts = [slice(j * cells, (j + 1) * cells) for j in range(slabs)]
    metric = [ej[0:1, cut] for cut in cuts]
    extent = [ej[8:9, cut] for cut in cuts]

    with scope("bar_wait"):
        pl.semaphore_wait(barrier, n - 1 + members - 1)
    with scope("send0"):
        exchange(0, parted(theta_s))
        (current_s,) = chosen_of(current)
        exchange(1, parted(current_s))

        for k in range(1, members):
            pl.semaphore_signal(ready_sem, inc=1, device_id=member_peer(k), device_id_type=MESH)

    with scope("g_build"):
        one_hot(g, (cells + halo) // LANES, slabs * cells, lambda cut: endj[0:1, cut])
    with scope("coef"):
        loads["v"].wait()
        for j in range(slabs):
            for b in range(blocks):
                lanes = slice(b * LANES, (b + 1) * LANES)
                wind = slab(v_ref, levels, b, j)
                down = extent[j][:, lanes] * (0.5 * wind - (0.5 * jnp.abs(wind) + kappa))
                cf[j, :, lanes] = down
                ct[j, :, lanes] = extent[j][:, lanes] * wind - down
    with scope("m3_build"):
        rows = [endj[0:1, cut].astype(F32) for cut in cuts] + [scale * m for m in metric]
        rows = jnp.concatenate(rows + [jnp.zeros((16 - 2 * slabs, cells), F32)], axis=0)
        y = fold(mm(halves(rows), pick[...]))
        for j in range(slabs):
            for at, part in enumerate(parted(y[j : j + 1])):
                lo = (at * slabs + j) * wide
                ends_s[0:1, lo : lo + wide] = part.astype(jnp.int32) - cells
        weight_s = [parted(y[slabs + j : slabs + j + 1]) for j in range(slabs)]
        one_hot(m3, nb, slabs * halo, lambda cut: ends_s[0:1, cut])

    def local(pressure, heat=None):
        lhs = [halves(pressure)] + ([] if heat is None else [halves(heat)])
        lhs = jnp.concatenate(lhs, axis=0)
        p_flux, t_flux = [], []
        for j in range(slabs):
            y = mm(lhs, g[:cells, cuts[j]])
            p_flux.append(metric[j] * (fold(y[: 2 * levels]) - pressure))
            if heat is not None:
                t_flux.append(cf[j] * fold(y[2 * levels :]) + ct[j] * heat)
        lhs = [halves(jnp.concatenate(p_flux, axis=1))]
        if heat is not None:
            lhs.append(halves(jnp.concatenate(t_flux, axis=1)))
        y = mm_nt(jnp.concatenate(lhs, axis=0), g[:cells, :])
        p_sum = sum(p_flux[1:], p_flux[0]) - fold(y[: 2 * levels])
        if heat is None:
            return p_sum
        return p_sum, sum(t_flux[1:], t_flux[0]) - fold(y[2 * levels :])

    def far(x, j):
        return mm(x, g[cells:, cuts[j]])

    def relay(slot, parts, weights, to=None):
        held = []
        parts = list(parts)
        for group, (lo, hi) in enumerate(spans):
            x = arrived(slot, group)
            held.append(x)
            found = []
            for part in range(groups):
                at = part * slabs * wide
                found.append(mm(x, m3[lo * hb : hi * hb, at : at + slabs * wide]))
            for part, y in enumerate(found):
                for j in range(slabs):
                    parts[part] = parts[part] + weights[j][part] * fold(
                        y[:, j * wide : (j + 1) * wide]
                    )
                if to is not None and hi == nb:
                    give(to, part, parts[part])
        return parts, jnp.concatenate(held, axis=1)

    def arrived_all(slot):
        return jnp.concatenate([arrived(slot, i) for i in range(len(spans))], axis=1)

    def heat_base(heat, div):
        step = heat[1:] - heat[:-1]
        zero = jnp.zeros((1, cells), F32)
        vertical = mixing * (
            jnp.concatenate([step, zero], 0) - jnp.concatenate([zero, step], 0)
        )
        return heat + jnp.where(owned, TIME_STEP * vertical, 0.0) - rate * div

    def lane_blocks(x):
        parts = [x[:, b * LANES : (b + 1) * LANES] for b in range(x.shape[1] // LANES)]
        return sum(parts[1:], parts[0])

    def partial_mean(slot, weighted):
        weighted = jnp.sum(weighted, axis=1, keepdims=True)
        whole = jnp.sum(area, axis=1, keepdims=True)
        row_at = lax.broadcasted_iota(jnp.int32, (levels, LANES), 0)
        lane_at = lax.broadcasted_iota(jnp.int32, (levels, LANES), 1)
        row = jnp.sum(jnp.where(row_at == lane_at, weighted, 0.0), axis=0, keepdims=True)
        lane = lax.broadcasted_iota(jnp.int32, (1, LANES), 1)
        row = jnp.where(lane < levels, row, whole)
        mean_send[slot] = jnp.broadcast_to(row, (8, LANES))
        for k in range(1, n):
            to_peer(
                mean_send.at[slot],
                mean_recv.at[slot, k - 1],
                mean_ssem.at[0],
                mean_rsem.at[slot],
                dom_peer(k),
            ).start()
        return row

    def mean_row(slot):
        to_peer(
            mean_recv.at[slot],
            mean_recv.at[slot],
            mean_ssem.at[0],
            mean_rsem.at[slot],
            dom_peer(1),
        ).wait_recv()
        total = mean_send[slot]
        for k in range(n - 1):
            total = total + mean_recv[slot, k]
        return total / total[:, levels : levels + 1]

    def as_column(row):
        row_at = lax.broadcasted_iota(jnp.int32, (levels, LANES), 0)
        lane_at = lax.broadcasted_iota(jnp.int32, (levels, LANES), 1)
        return jnp.sum(jnp.where(row_at == lane_at, row[0:1], 0.0), axis=1, keepdims=True)

    with scope("local_0"):
        p_sum, t_sum = local(current, theta)
        loads["q"].wait()
        base = jnp.where(owned, 2.0 * current - q_ref[0], current) + scale * p_sum
        t_base = heat_base(theta, t_sum)
    with scope("base_0"):
        base_s, t_base_s, *turn_s = chosen_of(
            base, t_base, *[-rate * cf[j] for j in range(slabs)]
        )
    share = couple / NS
    with scope("wait_0"):
        turn_s = [parted(x) for x in turn_s]
        t_out_s, out, theta_s = parted(t_base_s), parted(base_s), parted(theta_s)
        held = []
        for group, (lo, hi) in enumerate(spans):
            x = jnp.concatenate([arrived(0, group), arrived(1, group)], axis=0)
            held.append(x)
            found = []
            for part in range(groups):
                at = part * slabs * wide
                found.append(mm(x, m3[lo * hb : hi * hb, at : at + slabs * wide]))
            for part, y in enumerate(found):
                for j in range(slabs):
                    cut = slice(j * wide, (j + 1) * wide)
                    t_out_s[part] = t_out_s[part] + turn_s[j][part] * fold(y[: 2 * levels, cut])
                    out[part] = out[part] + weight_s[j][part] * fold(y[2 * levels :, cut])
                if hi == nb:
                    give(2, part, out[part] + share * (t_out_s[part] - theta_s[part]))
        exchange(STEPS * NS + 1, t_out_s)
        fence()
        both = jnp.concatenate(held, axis=1)
    with scope("full_0"):
        theta1 = t_base
        previous, stepped = current, base
        for j in range(slabs):
            y = far(both, j)
            theta1 = theta1 - rate * (cf[j] * fold(y[: 2 * levels]))
            stepped = stepped + (scale * metric[j]) * fold(y[2 * levels :])
        forcing = share * (theta1 - theta)
        current = stepped + forcing

    w_all = to_peer(w_send, w_recv, w_sem.at[0], w_sem.at[1], dom_peer(1))

    def pull(places):
        rows = jnp.concatenate([speed * m for m in metric], axis=1)
        rows = halves(jnp.broadcast_to(rows, (16, slabs * cells)))
        lo, hi = cells + places[0] * hb, cells + (places[-1] + 1) * hb
        w = fold(mm_nt(rows, g[lo:hi, :]))
        for i, u in enumerate(places):
            peer, place = in_from[u]
            w_send[u] = w[0:8, i * hb : (i + 1) * hb]
            to_peer(
                w_send.at[u], w_recv.at[place], w_sem.at[0], w_sem.at[1], peer
            ).start()

    layer = levels // members
    away = sorted(range(members), key=lambda x: (-bin(x).count("1"), x))

    def member_at(x):
        other = mine
        for stage in range(stages):
            if x >> stage & 1:
                bit = 1 << stage
                other = other + bit - 2 * bit * lax.rem(mine // bit, 2)
        return other
    en_all = to_peer(en_recv, en_recv, en_sem.at[0], en_sem.at[1], member_peer(1))
    eh_all = to_peer(eh, eh, en_sem.at[2], en_sem.at[3], dom_peer(1))

    def gather_exports(parts):
        for t in range(nb):
            at = t % GROUP * hb
            x = speed * parts[t // GROUP][:, at : at + hb]
            for m in range(members):
                en_send[m, t] = x[m * layer : (m + 1) * layer]
        for x in away[:-1]:
            to = member_at(x)
            to_peer(
                en_send.at[to], en_recv.at[x - 1], en_sem.at[0], en_sem.at[1], {"member": to}
            ).start()

    def spread_exports():
        if members > 1:
            en_all.wait_recv()
        summed = en_send[mine]
        for k in range(members - 1):
            summed = summed + en_recv[k]
        en_sum[...] = summed
        rows = pl.ds(pl.multiple_of(mine * layer, layer), layer)
        for t, (peer, place) in enumerate(out_to):
            for x in away:
                to_peer(
                    en_sum.at[t],
                    eh.at[place, rows],
                    en_sem.at[2],
                    en_sem.at[3],
                    {**peer, "member": member_at(x)},
                ).start()

    some = max(stages, 1)
    pieces = some * CHUNKS
    width = cells // pieces

    def member_copy(stage, c):
        return to_peer(
            mem_send.at[stage, c],
            mem_recv.at[stage, c],
            mem_ssem.at[0],
            mem_rsem.at[stage, c // some],
            partner((stage + c) % some),
        )

    def chunk_wait(stage, group):
        at = slice(group * some, (group + 1) * some)
        to_peer(
            mem_send.at[stage, at],
            mem_recv.at[stage, at],
            mem_ssem.at[0],
            mem_rsem.at[stage, group],
            partner(0),
        ).wait_recv()

    total = STEPS * NS
    for k in range(1, total):
        if k == total - 2 and members > 1:
            pl.semaphore_wait(ready_sem, members - 1)
        with scope(f"local_{k}"):
            if k == 1:
                p_sum, t_sum = local(current, theta1)
                t_base = heat_base(theta1, t_sum)
            else:
                p_sum = local(current)
            if k == NS:
                forcing = share * (theta2 - theta1)
                partial_mean(0, lane_blocks(current * area))
            base = (
                jnp.where(owned, 2.0 * current - previous, current) + scale * p_sum + forcing
            )
        if k < total - 1:
            with scope(f"base_{k}"):
                (base_s,) = chosen_of(base)
                base_s = parted(base_s)
        else:
            with scope("bulk"):
                for c in range(pieces):
                    mem_send[0, c] = base[:, c * width : (c + 1) * width]
                    if stages:
                        member_copy(0, c).start()
            with scope("mean_1"):
                w_all.wait_recv()
                weighted = lane_blocks(base * area)
                for b in range(nb):
                    weighted = weighted + w_recv[b, 0:1] * send[k + 1, b]
                mm_send[...] = partial_mean(1, weighted)
                for m in range(1, members):
                    for d in range(n):
                        to_peer(
                            mm_send,
                            mm_recv.at[m - 1, d],
                            mm_sem.at[0],
                            mm_sem.at[1],
                            {**dom_peer(d), **member_peer(m)},
                        ).start()
                first_row = mean_row(0)
                first = as_column(first_row)
            with scope("spread"):
                spread_exports()
        if k == NS - 1:
            with scope("heat_2"):
                ht = arrived_all(STEPS * NS + 1)
                theta2 = t_base
                for j in range(slabs):
                    theta2 = theta2 - rate * (cf[j] * fold(far(ht, j)))
                t_out[0] = theta2
                t_copy = pltpu.make_async_copy(t_out, t_hold, out_sem.at[0])
                t_copy.start()
        if k in (1, NS):
            with scope(f"pull_{k}"):
                pull(range(nb // 2) if k == 1 else range(nb // 2, nb))
        with scope(f"wait_{k}"):
            if k < total - 1:
                out, hp = relay(k + 1, base_s, weight_s, k + 2)
                if k == total - 2:
                    gather_exports(out)
                fence()
            else:
                hp = arrived_all(k + 1)
        with scope(f"full_{k}"):
            previous, stepped = current, base
            for j in range(slabs):
                stepped = stepped + (scale * metric[j]) * fold(far(hp, j))
            current = stepped

    for s in range(stages - 1):
        with scope(f"tail_stage_{s}"):
            for c in range(pieces):
                if c % some == 0:
                    chunk_wait(s, c // some)
                mem_send[s + 1, c] = mem_send[s, c] + mem_recv[s, c]
                member_copy(s + 1, c).start()
    with scope("tail_mean"):
        current = jnp.where(owned, current - first, current)
        last = mean_row(1) - first_row
        p_out[0] = jnp.where(owned, current - as_column(last), current)
        p_copy = pltpu.make_async_copy(p_out, p_hold, out_sem.at[1])
        p_copy.start()
    with scope("tail_far"):
        eh_all.wait_recv()
        x = halves(jnp.concatenate([eh[u] for u in range(nb)], axis=1))
        field = jnp.zeros((levels, cells), F32)
        for j in range(slabs):
            field = field + jnp.where(owned, inverse * metric[j], 0.0) * fold(far(x, j))
    with scope("tail_rows"):
        summed = (first_row + last)[0:1]
        if members > 1:
            to_peer(mm_recv, mm_recv, mm_sem.at[0], mm_sem.at[1], member_peer(1)).wait_recv()
            for m in range(members - 1):
                row = mm_recv[m, 0]
                for d in range(1, n):
                    row = row + mm_recv[m, d]
                summed = summed + row / row[:, levels : levels + 1]
        field = field - jnp.where(owned, as_column(summed), 0.0)
    with scope("tail_end"):
        for c in range(pieces):
            cut = slice(c * width, (c + 1) * width)
            x = mem_send[some - 1, c]
            if stages:
                if c % some == 0:
                    chunk_wait(stages - 1, c // some)
                x = x + mem_recv[stages - 1, c]
            e_out[:, cut] = (x + field[:, cut]) / members
        e_copy = pltpu.make_async_copy(e_out, e_hold, out_sem.at[2])
        e_copy.start()
    with scope("drain"):
        to_peer(send, recv, send_sem.at[0], recv_sem.at[0, 0], dom_peer(1)).wait_send()
        to_peer(mean_recv, mean_recv, mean_ssem.at[0], mean_rsem.at[0], dom_peer(1)).wait_send()
        w_all.wait_send()
        if members > 1:
            en_all.wait_send()
        eh_all.wait_send()
        if stages:
            to_peer(
                mem_send, mem_recv, mem_ssem.at[0], mem_rsem.at[0, 0], partner(0)
            ).wait_send()
        if members > 1:
            to_peer(mm_recv, mm_recv, mm_sem.at[0], mm_sem.at[1], member_peer(1)).wait_send()
        t_copy.wait()
        p_copy.wait()
        e_copy.wait()


def finish(p_hold, t_hold, e_hold, p_out, t_out, e_out, sem):
    copies = [
        pltpu.make_async_copy(src, dst, sem.at[at])
        for at, (src, dst) in enumerate(
            [(p_hold, p_out), (t_hold, t_out), (e_hold, e_out)]
        )
    ]
    for copy in copies:
        copy.start()
    for copy in copies:
        copy.wait()


def solution(mesh):
    n = mesh.shape["dom"]
    members = mesh.shape["member"]

    def per_device(
        acoustic_perturbation,
        prior_acoustic_state,
        thermal_anomaly,
        model_parameters,
        crossing_velocity,
        face_extent,
        face_metric_factor,
        reciprocal_polygon_surface,
        owned_totals,
        export_lists,
        face_neighbour_pair,
        polygon_side_lookup,
    ):
        _, levels, cells = acoustic_perturbation.shape
        edges = face_extent.shape[0]
        slabs = edges // cells
        nb, hb = export_lists.shape[1:]
        halo = nb * hb
        stages = members.bit_length() - 1
        some = max(stages, 1)
        pieces = some * CHUNKS
        slots = STEPS * NS + 2
        hbm = pl.BlockSpec(memory_space=pl.ANY)
        dma = pltpu.SemaphoreType.DMA
        field = pltpu.VMEM((1, levels, cells), F32)
        shapes = (
            jax.ShapeDtypeStruct((1, levels, cells), F32),
            jax.ShapeDtypeStruct((1, levels, cells), F32),
            jax.ShapeDtypeStruct((levels, cells), F32),
        )
        held = pl.pallas_call(
            functools.partial(kernel, n, members),
            out_shape=shapes,
            in_specs=[hbm] * 10,
            out_specs=(hbm, hbm, hbm),
            scratch_shapes=[
                pltpu.SMEM((1, 4), F32),
                field,
                field,
                pltpu.VMEM((levels, cells), F32),
                field,
                field,
                field,
                pltpu.VMEM((levels, edges), F32),
                pltpu.VMEM((1, edges), F32),
                pltpu.VMEM((1, edges), F32),
                pltpu.VMEM((1, cells), F32),
                pltpu.VMEM((1, halo), jnp.int32),
                pltpu.VMEM((2, edges), jnp.int32),
                dma((10,)),
                dma((3,)),
                pltpu.VMEM((1, halo), jnp.int32),
                pltpu.VMEM((cells, halo), F8),
                pltpu.VMEM((cells + halo, edges), F8),
                pltpu.VMEM((halo, slabs * halo), F8),
                pltpu.VMEM((16, edges), F32),
                pltpu.VMEM((8, edges), jnp.int32),
                pltpu.VMEM((16, edges), F32),
                pltpu.VMEM((8, edges), jnp.int32),
                pltpu.VMEM((8, slabs * halo), jnp.int32),
                pltpu.VMEM((slabs, levels, cells), F32),
                pltpu.VMEM((slabs, levels, cells), F32),
                pltpu.VMEM((slots, nb, levels, hb), F32),
                pltpu.VMEM((slots, nb, levels, hb), F32),
                pltpu.VMEM((STEPS, 8, LANES), F32),
                pltpu.VMEM((STEPS, n - 1, 8, LANES), F32),
                pltpu.VMEM((some, pieces, levels, cells // pieces), F32),
                pltpu.VMEM((some, pieces, levels, cells // pieces), F32),
                pltpu.VMEM((1, LANES), F32),
                pltpu.VMEM((max(members - 1, 1), n, 1, LANES), F32),
                pltpu.VMEM((nb, 8, hb), F32),
                pltpu.VMEM((nb, 8, hb), F32),
                pltpu.VMEM((members, nb, levels // members, hb), F32),
                pltpu.VMEM((max(members - 1, 1), nb, levels // members, hb), F32),
                pltpu.VMEM((nb, levels // members, hb), F32),
                pltpu.VMEM((nb, levels, hb), F32),
                dma((1,)),
                dma((4, 2)),
                dma((1,)),
                dma((STEPS,)),
                dma((1,)),
                dma((some, CHUNKS)),
                dma((2,)),
                dma((2,)),
                dma((4,)),
                pltpu.SemaphoreType.REGULAR,
                pltpu.SemaphoreType.REGULAR,
            ],
            compiler_params=pltpu.CompilerParams(
                collective_id=0, has_side_effects=True, vmem_limit_bytes=32 * 1024 * 1024
            ),
        )(
            *[
                pltpu.with_memory_space_constraint(x, pltpu.HBM)
                for x in (
                    model_parameters,
                    acoustic_perturbation,
                    prior_acoustic_state,
                    thermal_anomaly,
                    crossing_velocity,
                    face_extent[None],
                    face_metric_factor[None],
                    reciprocal_polygon_surface[None],
                    export_lists.reshape(1, halo),
                    face_neighbour_pair,
                )
            ],
        )
        return pl.pallas_call(
            finish,
            out_shape=shapes,
            in_specs=[hbm] * 3,
            out_specs=(hbm, hbm, hbm),
            scratch_shapes=[dma((3,))],
            compiler_params=pltpu.CompilerParams(vmem_limit_bytes=1024 * 1024),
        )(*held)

    in_specs = (
        P("member", None, "dom"),
        P("member", None, "dom"),
        P("member", None, "dom"),
        P("member", None),
        P(None, "dom"),
        P("dom"),
        P("dom"),
        P("dom"),
        P("dom"),
        P("dom", None, None),
        P(None, "dom"),
        P(None, "dom"),
    )
    out_specs = (P("member", None, "dom"), P("member", None, "dom"), P(None, "dom"))
    return jax.shard_map(
        per_device, mesh=mesh, in_specs=in_specs, out_specs=out_specs, check_vma=False
    )
```
